32 devices in a mesh: dp: 8 (over z, y), tensor: 4 (over x, core).
Axes of the slice: x: 2, y: 2, z: 4, core: 2. Of those that a mesh axis runs over, the one named last changes fastest.
Arguments:
- layer_input: bfloat16 [8192, 1536], P(('dp', 'tensor')), may hold values from -45 to 45
- text_states: bfloat16 [8, 64, 1536], P('dp'), may hold values from -6 to 6
- ln1_gain: float32 [1536], replicated, may hold values from 0.5 to 1.5
- ln1_bias: float32 [1536], replicated, may hold values from -1.5 to 1.5
- w_q: bfloat16 [1536, 1536], P(None, 'tensor'), may hold values from -0.15625 to 0.15625
- w_k: bfloat16 [1536, 1536], P(None, 'tensor'), may hold values from -0.15625 to 0.15625
- w_v: bfloat16 [1536, 1536], P(None, 'tensor'), may hold values from -0.15625 to 0.15625
- w_o: bfloat16 [1536, 1536], P('tensor'), may hold values from -0.625 to 0.625
- ln2_gain: float32 [1536], replicated, may hold values from 0.5 to 1.5
- ln2_bias: float32 [1536], replicated, may hold values from -1.5 to 1.5
- c_q: bfloat16 [1536, 1536], P(None, 'tensor'), may hold values from -0.15625 to 0.15625
- c_k: bfloat16 [1536, 1536], P(None, 'tensor'), may hold values from -0.15625 to 0.15625
- c_v: bfloat16 [1536, 1536], P(None, 'tensor'), may hold values from -0.15625 to 0.15625
- c_o: bfloat16 [1536, 1536], P('tensor'), may hold values from -0.625 to 0.625
- ln3_gain: float32 [1536], replicated, may hold values from 0.5 to 1.5
- ln3_bias: float32 [1536], replicated, may hold values from -1.5 to 1.5
- w_in: bfloat16 [1536, 6144], P(None, 'tensor'), may hold values from -0.15625 to 0.15625
- w_out: bfloat16 [6144, 1536], P('tensor'), may hold values from -0.078125 to 0.078125
- out_cotangent: bfloat16 [8192, 1536], P(('dp', 'tensor')), may hold values from -6 to 6
Outputs:
- block_out: bfloat16 [8192, 1536], P(('dp', 'tensor'))
- input_grad: bfloat16 [8192, 1536], P(('dp', 'tensor'))
- text_states_grad: bfloat16 [8, 64, 1536], P('dp', None, 'tensor')
- ln1_gain_grad: float32 [1536], replicated
- ln1_bias_grad: float32 [1536], replicated
- w_q_grad: float32 [1536, 1536], P('dp', 'tensor')
- w_k_grad: float32 [1536, 1536], P('dp', 'tensor')
- w_v_grad: float32 [1536, 1536], P('dp', 'tensor')
- w_o_grad: float32 [1536, 1536], P('tensor', 'dp')
- ln2_gain_grad: float32 [1536], replicated
- ln2_bias_grad: float32 [1536], replicated
- c_q_grad: float32 [1536, 1536], P('dp', 'tensor')
- c_k_grad: float32 [1536, 1536], P('dp', 'tensor')
- c_v_grad: float32 [1536, 1536], P('dp', 'tensor')
- c_o_grad: float32 [1536, 1536], P('tensor', 'dp')
- ln3_gain_grad: float32 [1536], replicated
- ln3_bias_grad: float32 [1536], replicated
- w_in_grad: float32 [1536, 6144], P('dp', 'tensor')
- w_out_grad: float32 [6144, 1536], P('tensor', 'dp')
- root_squares: float32 [4], replicated
The draws below stay inside these ranges and needn't reach their ends.
All inputs are finite; a program needn't handle non-finite values.
Results may differ from the reference program's by a relative error of at most 0.022.
Values may be sent and summed in bfloat16 or wider, within the bound.
A program may use at most 192 MiB of HBM per device.

```python
import jax
import jax.numpy as jnp
from jax import lax

D = 1536
H = 24
HD = 64
FF = 6144
TEXT = 64
FRAMES = 1024
CLIPS = 8
TOKENS = 8192


def draw_layer_input(key, part):
    row_pos = jnp.arange(TOKENS, dtype=jnp.float32)[:, None]
    row_scale = jnp.exp(jnp.log(3.0) * row_pos / TOKENS)
    base_vals = jnp.clip(jax.random.normal(key, (TOKENS, D), jnp.float32), -5.0, 5.0)
    return (base_vals * row_scale).astype(jnp.bfloat16)


def with_spikes(values, stream_key, source, target, blocks, factor):
    owner, partner = [(jnp.arange(values.shape[axis_at]) // (values.shape[axis_at] // blocks)).reshape([-1 if axis == axis_at else 1 for axis in range(values.ndim)]) for axis_at in (source, target)]
    chosen = jax.random.permutation(stream_key, blocks)[partner]
    strong = (owner == chosen) | (owner == (partner + blocks // 2) % blocks)
    return jnp.where(strong, factor * values, values)


def shard_levels(stream_key, dims, pieces, least, largest):
    factor_of, own = 1.0, jax.random.fold_in(stream_key, 6)
    for axis_at, shards_of in pieces:
        steps = jnp.exp(jax.random.uniform(jax.random.fold_in(own, axis_at), (shards_of,), jnp.float32, least / len(pieces), largest / len(pieces)))
        factor_of = factor_of * jnp.repeat(steps, dims[axis_at] // shards_of).reshape([-1 if axis == axis_at else 1 for axis in range(len(dims))])
    return factor_of


def scatter_about(stream_key, dims, scale, most, cuts=(), kind=jnp.bfloat16):
    factor_of = shard_levels(stream_key, dims, cuts, -0.22, 0.18) if cuts else 1.0
    entries = jax.random.normal(stream_key, dims, jnp.float32) * scale * factor_of
    return jnp.minimum(jnp.maximum(entries, -most), most).astype(kind)


def heavy_noise(key, extent, width, limit, split, heavy, kind=jnp.bfloat16):
    drawn = width * jax.random.normal(key, extent, jnp.float32)
    if split:
        drawn = drawn * shard_levels(key, extent, split, -0.22, 0.18)
    return jnp.clip(with_spikes(drawn, jax.random.fold_in(key, 3), *heavy), -limit, limit).astype(kind)


def setup_inputs(seed: int = 0) -> dict:
    splits = jax.random.split(jax.random.key(seed), 20)
    layer_input = draw_layer_input(jax.random.fold_in(splits[19], 71), 0)
    text_states = scatter_about(splits[1], (CLIPS, TEXT, D), 1.0, 6.0, ((0, 8),))
    ln1_gain = jnp.clip(1.0 + 0.1 * jax.random.normal(splits[2], (D,), jnp.float32), 0.5, 1.5)
    ln1_bias = scatter_about(splits[3], (D,), 0.3, 1.5, (), jnp.float32)
    w_q = scatter_about(splits[4], (D, D), D ** -0.5, 0.15625, ((1, 4),))
    w_k = scatter_about(splits[5], (D, D), D ** -0.5, 0.15625, ((1, 4),))
    w_v = scatter_about(splits[6], (D, D), D ** -0.5, 0.15625, ((1, 4),))
    w_o = scatter_about(splits[7], (D, D), (D // 16) ** -0.5, 0.625, ((0, 4),))
    ln2_gain = jnp.clip(1.0 + 0.1 * jax.random.normal(splits[8], (D,), jnp.float32), 0.5, 1.5)
    ln2_bias = scatter_about(splits[9], (D,), 0.3, 1.5, (), jnp.float32)
    c_q = scatter_about(splits[10], (D, D), D ** -0.5, 0.15625, ((1, 4),))
    c_k = scatter_about(splits[11], (D, D), D ** -0.5, 0.15625, ((1, 4),))
    c_v = scatter_about(splits[12], (D, D), D ** -0.5, 0.15625, ((1, 4),))
    c_o = scatter_about(splits[13], (D, D), (D // 16) ** -0.5, 0.625, ((0, 4),))
    ln3_gain = jnp.clip(1.0 + 0.1 * jax.random.normal(splits[14], (D,), jnp.float32), 0.5, 1.5)
    ln3_bias = scatter_about(splits[15], (D,), 0.3, 1.5, (), jnp.float32)
    w_in = scatter_about(splits[16], (D, FF), D ** -0.5, 0.15625, ((1, 4),))
    w_out = scatter_about(splits[17], (FF, D), FF ** -0.5, 0.078125, ((0, 4),))
    out_cotangent = heavy_noise(splits[18], (TOKENS, D), 1.0, 6.0, ((0, 32),), (0, 1, 32, 2.75))
    return {"layer_input": layer_input, "text_states": text_states, "ln1_gain": ln1_gain, "ln1_bias": ln1_bias, "w_q": w_q, "w_k": w_k, "w_v": w_v, "w_o": w_o, "ln2_gain": ln2_gain, "ln2_bias": ln2_bias, "c_q": c_q, "c_k": c_k, "c_v": c_v, "c_o": c_o, "ln3_gain": ln3_gain, "ln3_bias": ln3_bias, "w_in": w_in, "w_out": w_out, "out_cotangent": out_cotangent}


@jax.custom_vjp
def low(v):
    return lax.optimization_barrier(v.astype(jnp.bfloat16)).astype(jnp.float32)

@jax.custom_vjp
def low_back(v):
    return v

def low_keep(v):
    return (low(v), None)

def low_pass(kept, grad):
    return (grad,)

def back_keep(v):
    return (v, None)

def back_low(kept, grad):
    return (low(grad),)
low.defvjp(low_keep, low_pass)
low_back.defvjp(back_keep, back_low)
norm_eps = 1e-05
highest = lax.Precision.HIGHEST

def both_low(values):
    return low_back(low(values))

def layer_norm(stream, gain_vec, shift_vec):
    centre = lax.optimization_barrier(jnp.mean(stream, axis=-1, keepdims=True))
    centred = stream - centre
    spread = lax.optimization_barrier(jnp.mean(centred * centred, axis=-1, keepdims=True))
    return centred * lax.rsqrt(spread + norm_eps) * gain_vec + shift_vec

def product(left_mat, right_mat):
    return jnp.dot(left_mat, right_mat, precision=highest, preferred_element_type=jnp.float32)

def attention(queries, all_keys, all_values, causal):
    query_len = queries.shape[0]
    key_len = all_keys.shape[0]
    query_heads = queries.reshape(query_len, H, HD)
    key_heads = all_keys.reshape(key_len, H, HD)
    value_heads = all_values.reshape(key_len, H, HD)
    scores = low_back(jnp.einsum('qhd,khd->hqk', query_heads, key_heads, precision=highest) * HD ** (-0.5))
    if causal:
        row_ids = lax.broadcasted_iota(jnp.int32, (query_len, key_len), 0)
        col_ids = lax.broadcasted_iota(jnp.int32, (query_len, key_len), 1)
        scores = jnp.where((col_ids <= row_ids)[None], scores, -1e+30)
    weights = low(jax.nn.softmax(scores, axis=-1))
    mixed_out = jnp.einsum('hqk,khd->qhd', weights, value_heads, precision=highest)
    return both_low(mixed_out.reshape(query_len, H * HD))

def clip_forward(params, clip_rows, clip_text):
    gain_one, bias_one, wq_mat, wk_mat, wv_mat, wo_mat, gain_two, bias_two, cq_mat, ck_mat, cv_mat, co_mat, gain_three, bias_three, win_mat, wout_mat = params
    normed = low(layer_norm(clip_rows, gain_one, bias_one))
    attended = attention(both_low(product(normed, wq_mat)), both_low(product(normed, wk_mat)), both_low(product(normed, wv_mat)), True)
    branch_one = low_back(product(attended, wo_mat))
    hidden_one = clip_rows + branch_one
    normed = low(layer_norm(hidden_one, gain_two, bias_two))
    crossed = attention(both_low(product(normed, cq_mat)), both_low(product(clip_text, ck_mat)), both_low(product(clip_text, cv_mat)), False)
    branch_two = low_back(product(crossed, co_mat))
    hidden_two = hidden_one + branch_two
    normed = low(layer_norm(hidden_two, gain_three, bias_three))
    pre_act = low_back(product(normed, win_mat))
    branch_three = low_back(product(low(jax.nn.gelu(pre_act, approximate=False)), wout_mat))
    block_out = hidden_two + branch_three
    squares = jnp.stack([jnp.sum(clip_rows * clip_rows), jnp.sum(branch_one * branch_one), jnp.sum(branch_two * branch_two), jnp.sum(branch_three * branch_three)])
    return (block_out, squares)

def forward_all(stream, text_rows, *params):

    def one_clip(params_in, clip_pair):
        return clip_forward(params_in, clip_pair[0], clip_pair[1])
    checked = jax.checkpoint(one_clip)
    outputs, squares = lax.map(lambda clip_pair: checked(params, clip_pair), (stream.reshape(CLIPS, FRAMES, D), text_rows))
    return (outputs.reshape(TOKENS, D), lax.optimization_barrier(jnp.sum(squares, axis=0)))

def reference(layer_input, text_states, ln1_gain, ln1_bias, w_q, w_k, w_v, w_o, ln2_gain, ln2_bias, c_q, c_k, c_v, c_o, ln3_gain, ln3_bias, w_in, w_out, out_cotangent):
    primals = [entry.astype(jnp.float32) for entry in (layer_input, text_states, ln1_gain, ln1_bias, w_q, w_k, w_v, w_o, ln2_gain, ln2_bias, c_q, c_k, c_v, c_o, ln3_gain, ln3_bias, w_in, w_out)]
    block_out, pullback, squares = jax.vjp(forward_all, *primals, has_aux=True)
    all_grads = pullback(out_cotangent.astype(jnp.float32))
    root_squares = jnp.sqrt(squares / (TOKENS * D))
    return (block_out.astype(jnp.bfloat16), all_grads[0].astype(jnp.bfloat16), all_grads[1].astype(jnp.bfloat16), all_grads[2], all_grads[3], all_grads[4], all_grads[5], all_grads[6], all_grads[7], all_grads[8], all_grads[9], all_grads[10], all_grads[11], all_grads[12], all_grads[13], all_grads[14], all_grads[15], all_grads[16], all_grads[17], root_squares)
```

```python
from functools import partial

import jax
import jax.numpy as jnp
from jax import lax
from jax.sharding import PartitionSpec as P

HD = 64
FRAMES = 1024


norm_eps = 1e-05


def layer_norm(stream, gain_vec, shift_vec):
    centre = jnp.mean(stream, axis=-1, keepdims=True)
    centred = stream - centre
    spread = jnp.mean(centred * centred, axis=-1, keepdims=True)
    return centred * lax.rsqrt(spread + norm_eps) * gain_vec + shift_vec


def product(left_mat, right_mat):
    return jnp.dot(left_mat, right_mat, preferred_element_type=jnp.float32)


def contract_rows(left_mat, right_mat):
    return lax.dot_general(
        left_mat, right_mat, (((0,), (0,)), ((), ())), preferred_element_type=jnp.float32
    )


def contract_cols(left_mat, right_mat):
    return lax.dot_general(
        left_mat, right_mat, (((1,), (1,)), ((), ())), preferred_element_type=jnp.float32
    )


def exchange(values, flip):
    return lax.ppermute(values, "tensor", [(i, i ^ flip) for i in range(4)])


def gather_relative(values):
    far = exchange(values, 2)
    return values, exchange(values, 1), far, exchange(far, 1)


def scatter_relative(near_own, near_other, far_mine, far_other):
    over_link = exchange(far_mine + exchange(far_other, 1), 2)
    return near_own.astype(jnp.float32) + exchange(near_other, 1) + over_link


def swap_relative(blocks):
    return [blocks[0]] + [exchange(blocks[flip], flip) for flip in (1, 2, 3)]


def to_absolute(values, own_id):
    rows = values.shape[0] // 4
    return jnp.concatenate(
        [lax.dynamic_slice_in_dim(values, (own_id ^ flip) * rows, rows, 0) for flip in range(4)]
    )


def scatter_product(far_pair, near_pair, own_rows):
    far_part = far_pair().astype(jnp.bfloat16)
    mine, other = far_part[:own_rows], far_part[own_rows:]
    over_link = exchange(mine + exchange(other, 1), 2)
    near_part = near_pair()
    near_other = exchange(near_part[own_rows:].astype(jnp.bfloat16), 1)
    return near_part[:own_rows] + near_other + over_link


def sum_clips(part):
    size = lax.axis_size("dp")
    if size != 8:
        return lax.psum_scatter(
            part.astype(jnp.bfloat16), "dp", scatter_dimension=0, tiled=True
        ).astype(jnp.float32)
    own = lax.axis_index("dp")
    own_z, own_y = own // 2, own % 2
    rows = part.shape[0] // 8
    halves = part.astype(jnp.bfloat16).reshape(4, 2, rows, part.shape[1])
    sent = lax.dynamic_index_in_dim(halves, 1 - own_y, 1, keepdims=False)
    kept = lax.dynamic_index_in_dim(halves, own_y, 1, keepdims=False)
    kept = kept + lax.ppermute(sent, "dp", [(i, i ^ 1) for i in range(8)])
    total = lax.dynamic_index_in_dim(kept, own_z, 0, keepdims=False).astype(jnp.float32)
    for sign in (1, -1):
        carried = None
        for step in range(1, 4):
            target = jnp.clip(own_z + sign * (4 - step), 0, 3)
            block = lax.dynamic_index_in_dim(kept, target, 0, keepdims=False)
            if carried is not None:
                block = block + carried
            senders = range(step) if sign > 0 else range(3, 3 - step, -1)
            pairs = [(2 * z + y, 2 * (z + sign) + y) for z in senders for y in range(2)]
            carried = lax.ppermute(block, "dp", pairs)
        total = total + carried
    return total


def sum_everywhere(values):
    if lax.axis_size("dp") != 8:
        return lax.psum(values, ("dp", "tensor"))
    for flip in (1, 2):
        values = values + exchange(values, flip)
    for flip in (1, 2, 4):
        values = values + lax.ppermute(values, "dp", [(i, i ^ flip) for i in range(8)])
    return values


def after(values, *others):
    return lax.optimization_barrier((values,) + others)[0]


def block_scores(queries, all_keys, begin_row, end_row):
    scores = jnp.einsum(
        "cqhd,ckhd->chqk",
        queries[:, begin_row:end_row],
        all_keys[:, :end_row],
        preferred_element_type=jnp.float32,
    ) * HD ** (-0.5)
    row_ids = begin_row + lax.broadcasted_iota(jnp.int32, (end_row - begin_row, end_row), 0)
    col_ids = lax.broadcasted_iota(jnp.int32, (end_row - begin_row, end_row), 1)
    return jnp.where(col_ids <= row_ids, scores, -1e30)


def self_forward(queries, all_keys, all_values):
    block_rows = min(512, FRAMES)
    outputs, peak_list, sum_list = ([], [], [])
    for begin_row in range(0, FRAMES, block_rows):
        end_row = begin_row + block_rows
        scores = block_scores(queries, all_keys, begin_row, end_row)
        row_peak = jnp.max(scores, axis=-1, keepdims=True)
        exp_scores = jnp.exp(scores - row_peak)
        row_sum = jnp.sum(exp_scores, axis=-1, keepdims=True)
        weights = (exp_scores / row_sum).astype(jnp.bfloat16)
        outputs.append(
            jnp.einsum(
                "chqk,ckhd->cqhd",
                weights,
                all_values[:, :end_row],
                preferred_element_type=jnp.float32,
            )
        )
        peak_list.append(row_peak)
        sum_list.append(row_sum)
    return (jnp.concatenate(outputs, axis=1), peak_list, sum_list)


def self_backward(queries, all_keys, all_values, peak_list, sum_list, grad_mixed):
    block_rows = min(512, FRAMES)
    score_scale = HD ** (-0.5)
    query_parts = []
    grad_keys = jnp.zeros(all_keys.shape, jnp.float32)
    grad_values = jnp.zeros(all_values.shape, jnp.float32)
    for block_id, begin_row in enumerate(range(0, FRAMES, block_rows)):
        end_row = begin_row + block_rows
        scores = block_scores(queries, all_keys, begin_row, end_row)
        weights = jnp.exp(scores - peak_list[block_id]) / sum_list[block_id]
        grad_weights = jnp.einsum(
            "cqhd,ckhd->chqk",
            grad_mixed[:, begin_row:end_row],
            all_values[:, :end_row],
            preferred_element_type=jnp.float32,
        )
        row_dot = jnp.sum(weights * grad_weights, axis=-1, keepdims=True)
        grad_scores = (weights * (grad_weights - row_dot)).astype(jnp.bfloat16)
        query_parts.append(
            jnp.einsum(
                "chqk,ckhd->cqhd",
                grad_scores,
                all_keys[:, :end_row],
                preferred_element_type=jnp.float32,
            )
            * score_scale
        )
        grad_keys = grad_keys.at[:, :end_row].add(
            jnp.einsum(
                "chqk,cqhd->ckhd",
                grad_scores,
                queries[:, begin_row:end_row],
                preferred_element_type=jnp.float32,
            )
            * score_scale
        )
        grad_values = grad_values.at[:, :end_row].add(
            jnp.einsum(
                "chqk,cqhd->ckhd",
                weights.astype(jnp.bfloat16),
                grad_mixed[:, begin_row:end_row],
                preferred_element_type=jnp.float32,
            )
        )
    return (jnp.concatenate(query_parts, axis=1), grad_keys, grad_values)


def cross_forward(queries, all_keys, all_values):
    scores = jnp.einsum(
        "cqhd,ckhd->chqk", queries, all_keys, preferred_element_type=jnp.float32
    ) * HD ** (-0.5)
    row_peak = jnp.max(scores, axis=-1, keepdims=True)
    exp_scores = jnp.exp(scores - row_peak)
    weights = exp_scores / jnp.sum(exp_scores, axis=-1, keepdims=True)
    mixed_out = jnp.einsum(
        "chqk,ckhd->cqhd",
        weights.astype(jnp.bfloat16),
        all_values,
        preferred_element_type=jnp.float32,
    )
    return (mixed_out, weights)


def cross_backward(queries, all_keys, all_values, weights, grad_mixed):
    score_scale = HD ** (-0.5)
    grad_weights = jnp.einsum(
        "cqhd,ckhd->chqk", grad_mixed, all_values, preferred_element_type=jnp.float32
    )
    row_dot = jnp.sum(weights * grad_weights, axis=-1, keepdims=True)
    grad_scores = (weights * (grad_weights - row_dot)).astype(jnp.bfloat16)
    grad_queries = (
        jnp.einsum("chqk,ckhd->cqhd", grad_scores, all_keys, preferred_element_type=jnp.float32)
        * score_scale
    )
    grad_keys = (
        jnp.einsum("chqk,cqhd->ckhd", grad_scores, queries, preferred_element_type=jnp.float32)
        * score_scale
    )
    grad_values = jnp.einsum(
        "chqk,cqhd->ckhd",
        weights.astype(jnp.bfloat16),
        grad_mixed,
        preferred_element_type=jnp.float32,
    )
    return (grad_queries, grad_keys, grad_values)


def body(
    layer_input,
    text_states,
    ln1_gain,
    ln1_bias,
    w_q,
    w_k,
    w_v,
    w_o,
    ln2_gain,
    ln2_bias,
    c_q,
    c_k,
    c_v,
    c_o,
    ln3_gain,
    ln3_bias,
    w_in,
    w_out,
    out_cotangent,
):
    clip_count = text_states.shape[0]
    text_len = text_states.shape[1]
    own_rows, model_width = layer_input.shape
    local_width = w_q.shape[1]
    local_heads = local_width // HD
    own_id = lax.axis_index("tensor")
    low = jnp.bfloat16

    def split_heads(matrix, length):
        return matrix.astype(low).reshape(1, length, matrix.shape[1] // HD, HD)

    def merge_heads(tensor_four):
        return tensor_four.reshape(tensor_four.shape[1], -1).astype(low)

    stream = layer_input.astype(jnp.float32)
    normed_one = layer_norm(stream, ln1_gain, ln1_bias).astype(low)
    one = gather_relative(normed_one)
    w_qkv = jnp.concatenate([w_q, w_k, w_v], axis=1)
    near_one = jnp.concatenate(one[:2])
    far_one = jnp.concatenate(one[2:])
    rows_one = jnp.concatenate([near_one, far_one])
    qkv = jnp.concatenate(
        [product(near_one, w_qkv).astype(low), product(far_one, w_qkv).astype(low)]
    )
    qkv = to_absolute(qkv, own_id)
    queries, all_keys, all_values = [
        split_heads(qkv[:, i * local_width : (i + 1) * local_width], FRAMES) for i in range(3)
    ]
    mixed_one, peak_list, sum_list = self_forward(queries, all_keys, all_values)
    attended = to_absolute(merge_heads(mixed_one), own_id)
    branch_one = scatter_product(
        lambda: product(attended[2 * own_rows :], w_o),
        lambda: product(attended[: 2 * own_rows], w_o),
        own_rows,
    )

    c_q_full = jnp.concatenate(gather_relative(after(c_q, one[2])), axis=1)
    c_o_full = jnp.concatenate(gather_relative(after(c_o, one[2])), axis=0)
    text_rows = text_states.reshape(clip_count * text_len, model_width)
    text_kv = after(
        jnp.concatenate([product(text_rows, c_k), product(text_rows, c_v)]).astype(low), one[2]
    )
    text_kv = jnp.concatenate(gather_relative(text_kv), axis=1)
    text_keys = split_heads(text_kv[:text_len], text_len)
    text_values = split_heads(text_kv[text_len:], text_len)
    grad_rows = gather_relative(after(out_cotangent, c_o_full))
    grad_near = jnp.concatenate(grad_rows[:2])
    grad_far = jnp.concatenate(grad_rows[2:])
    grad_three_rows = jnp.concatenate([grad_near, grad_far])

    hidden_one = stream + branch_one
    normed_two = layer_norm(hidden_one, ln2_gain, ln2_bias).astype(low)
    cross_queries = split_heads(product(normed_two, c_q_full), own_rows)
    mixed_two, cross_weights = cross_forward(cross_queries, text_keys, text_values)
    crossed = merge_heads(mixed_two)
    branch_two = product(crossed, c_o_full)
    hidden_two = hidden_one + branch_two
    normed_three = layer_norm(hidden_two, ln3_gain, ln3_bias).astype(low)

    three = gather_relative(normed_three)
    near_three = jnp.concatenate(three[:2])
    far_three = jnp.concatenate(three[2:])
    act_parts, pre_grads = [], []
    for rows, grads in ((near_three, grad_near), (far_three, grad_far)):
        pre_act = product(rows, w_in)
        gelu_value, gelu_back = jax.vjp(partial(jax.nn.gelu, approximate=False), pre_act)
        act_parts.append(gelu_value.astype(low))
        pre_grads.append(gelu_back(contract_cols(grads, w_out))[0].astype(low))
    grad_normed_three = scatter_product(
        lambda: contract_cols(pre_grads[1], w_in),
        lambda: contract_cols(pre_grads[0], w_in),
        own_rows,
    )
    rows_three = jnp.concatenate([near_three, far_three])
    activated = jnp.concatenate(act_parts)
    grad_pre = jnp.concatenate(pre_grads)
    w_out_part = contract_rows(grad_three_rows, activated)
    w_in_part = contract_rows(rows_three, grad_pre)
    w_out_grad = sum_clips(w_out_part).T
    w_in_grad = sum_clips(w_in_part)
    branch_three = scatter_product(
        lambda: product(after(act_parts[1], grad_normed_three), w_out),
        lambda: product(act_parts[0], w_out),
        own_rows,
    )
    block_out = (hidden_two + branch_three).astype(low)
    squares = jnp.stack(
        [
            jnp.sum(stream * stream),
            jnp.sum(branch_one * branch_one),
            jnp.sum(branch_two * branch_two),
            jnp.sum(branch_three * branch_three),
        ]
    )

    grad_out = out_cotangent.astype(jnp.float32)
    norm_value, norm_back = jax.vjp(layer_norm, hidden_two, ln3_gain, ln3_bias)
    back_rows, ln3_gain_part, ln3_bias_part = norm_back(grad_normed_three)
    grad_two = grad_out + back_rows
    grad_two_low = grad_two.astype(low)
    grad_mixed_two = split_heads(contract_cols(grad_two_low, c_o_full), own_rows)
    grad_cq, grad_tk, grad_tv = cross_backward(
        cross_queries, text_keys, text_values, cross_weights, grad_mixed_two
    )
    grad_cq = merge_heads(grad_cq)
    grad_normed_two = contract_cols(grad_cq, c_q_full)
    norm_value, norm_back = jax.vjp(layer_norm, hidden_one, ln2_gain, ln2_bias)
    back_rows, ln2_gain_part, ln2_bias_part = norm_back(grad_normed_two)
    grad_one = grad_two + back_rows

    one_grads = gather_relative(grad_one.astype(low))
    grad_one_rows = jnp.concatenate(one_grads)
    grad_mixed_one = jnp.concatenate(
        [
            contract_cols(jnp.concatenate(one_grads[:2]), w_o).astype(low),
            contract_cols(jnp.concatenate(one_grads[2:]), w_o).astype(low),
        ]
    )
    grad_mixed_one = split_heads(to_absolute(grad_mixed_one, own_id), FRAMES)
    grad_sq, grad_sk, grad_sv = self_backward(
        queries, all_keys, all_values, peak_list, sum_list, grad_mixed_one
    )
    grad_qkv = jnp.concatenate([merge_heads(part) for part in (grad_sq, grad_sk, grad_sv)], axis=1)
    grad_qkv = to_absolute(grad_qkv, own_id)
    grad_normed_one = scatter_product(
        lambda: contract_cols(grad_qkv[2 * own_rows :], w_qkv),
        lambda: contract_cols(grad_qkv[: 2 * own_rows], w_qkv),
        own_rows,
    )
    qkv_grad = sum_clips(contract_rows(rows_one, grad_qkv))
    w_q_grad, w_k_grad, w_v_grad = jnp.split(qkv_grad, 3, axis=1)
    norm_value, norm_back = jax.vjp(layer_norm, stream, ln1_gain, ln1_bias)
    back_rows, ln1_gain_part, ln1_bias_part = norm_back(grad_normed_one)
    input_grad = (grad_one + back_rows).astype(low)

    def columns(matrix):
        return [matrix[:, i * local_width : (i + 1) * local_width] for i in range(4)]

    rows_two = jnp.concatenate(gather_relative(after(normed_two, one_grads[2])))
    grad_two_rows = jnp.concatenate(gather_relative(after(grad_two_low, one_grads[2])))
    crossed_rows = jnp.concatenate(swap_relative(columns(after(crossed, one_grads[2]))))
    grad_cq_rows = jnp.concatenate(swap_relative(columns(after(grad_cq, one_grads[2]))))
    grad_text = jnp.concatenate(
        [part.reshape(text_len, -1) for part in (grad_tk, grad_tv)]
    ).astype(jnp.float32)
    grad_text = scatter_relative(*columns(grad_text)).astype(low)
    grad_tk, grad_tv = grad_text[:text_len], grad_text[text_len:]
    cross_grad = sum_clips(
        jnp.concatenate(
            [
                contract_rows(grad_two_rows, crossed_rows).astype(low),
                contract_rows(rows_two, grad_cq_rows).astype(low),
                contract_rows(text_rows, grad_tk).astype(low),
                contract_rows(text_rows, grad_tv).astype(low),
                contract_rows(grad_one_rows, attended).astype(low),
            ],
            axis=1,
        )
    )
    c_o_grad, c_q_grad, c_k_grad, c_v_grad, w_o_grad = jnp.split(cross_grad, 5, axis=1)
    c_o_grad, w_o_grad = c_o_grad.T, w_o_grad.T
    text_term = (contract_cols(grad_tk, c_k) + contract_cols(grad_tv, c_v)).astype(low)
    text_states_grad = (
        scatter_relative(
            *[
                lax.dynamic_slice_in_dim(text_term, (own_id ^ flip) * local_width, local_width, 1)
                for flip in range(4)
            ]
        )
        .astype(low)
        .reshape(clip_count, text_len, local_width)
    )

    early = sum_everywhere(
        jnp.concatenate(
            [ln3_gain_part, ln3_bias_part, ln2_gain_part, ln2_bias_part, jnp.pad(squares, (0, 124))]
        )
    )
    late = sum_everywhere(jnp.concatenate([ln1_gain_part, ln1_bias_part]))
    ln3_gain_grad, ln3_bias_grad, ln2_gain_grad, ln2_bias_grad = [
        early[i * model_width : (i + 1) * model_width] for i in range(4)
    ]
    ln1_gain_grad, ln1_bias_grad = late[:model_width], late[model_width:]
    square_totals = early[4 * model_width : 4 * model_width + 4]
    entry_count = own_rows * lax.axis_size("dp") * lax.axis_size("tensor") * model_width
    root_squares = jnp.sqrt(square_totals / entry_count)
    return (
        block_out,
        input_grad,
        text_states_grad,
        ln1_gain_grad,
        ln1_bias_grad,
        w_q_grad,
        w_k_grad,
        w_v_grad,
        w_o_grad,
        ln2_gain_grad,
        ln2_bias_grad,
        c_q_grad,
        c_k_grad,
        c_v_grad,
        c_o_grad,
        ln3_gain_grad,
        ln3_bias_grad,
        w_in_grad,
        w_out_grad,
        root_squares,
    )


def solution(mesh):
    return jax.shard_map(
        body,
        mesh=mesh,
        in_specs=(
            P(("dp", "tensor"), None),
            P("dp", None, None),
            P(),
            P(),
            P(None, "tensor"),
            P(None, "tensor"),
            P(None, "tensor"),
            P("tensor", None),
            P(),
            P(),
            P(None, "tensor"),
            P(None, "tensor"),
            P(None, "tensor"),
            P("tensor", None),
            P(),
            P(),
            P(None, "tensor"),
            P("tensor", None),
            P(("dp", "tensor"), None),
        ),
        out_specs=(
            P(("dp", "tensor"), None),
            P(("dp", "tensor"), None),
            P("dp", None, "tensor"),
            P(),
            P(),
            P("dp", "tensor"),
            P("dp", "tensor"),
            P("dp", "tensor"),
            P("tensor", "dp"),
            P(),
            P(),
            P("dp", "tensor"),
            P("dp", "tensor"),
            P("dp", "tensor"),
            P("tensor", "dp"),
            P(),
            P(),
            P("dp", "tensor"),
            P("tensor", "dp"),
            P(),
        ),
        check_vma=False,
    )
```

```python
from functools import partial

import jax
import jax.numpy as jnp
from jax import lax
from jax.experimental import pallas as pl
from jax.experimental.pallas import tpu as pltpu
from jax.sharding import PartitionSpec as P


HD = 64


norm_eps = 1e-05


def layer_norm(stream, gain_vec, shift_vec):
    centre = jnp.mean(stream, axis=-1, keepdims=True)
    centred = stream - centre
    spread = jnp.mean(centred * centred, axis=-1, keepdims=True)
    return centred * lax.rsqrt(spread + norm_eps) * gain_vec + shift_vec


def product(left_mat, right_mat):
    return jnp.dot(left_mat, right_mat, preferred_element_type=jnp.float32)


def contract_rows(left_mat, right_mat):
    return lax.dot_general(
        left_mat, right_mat, (((0,), (0,)), ((), ())), preferred_element_type=jnp.float32
    )


def contract_cols(left_mat, right_mat):
    return lax.dot_general(
        left_mat, right_mat, (((1,), (1,)), ((), ())), preferred_element_type=jnp.float32
    )


def exchange(values, flip):
    return lax.ppermute(values, "tensor", [(i, i ^ flip) for i in range(4)])


def gather_relative(values):
    far = exchange(values, 2)
    return values, exchange(values, 1), far, exchange(far, 1)


def scatter_relative(near_own, near_other, far_mine, far_other):
    over_link = exchange(far_mine + exchange(far_other, 1), 2)
    return near_own.astype(jnp.float32) + exchange(near_other, 1) + over_link


def swap_relative(blocks):
    return [blocks[0]] + [exchange(blocks[flip], flip) for flip in (1, 2, 3)]


def scatter_product(far_pair, near_pair, own_rows):
    far_part = far_pair().astype(jnp.bfloat16)
    mine, other = far_part[:own_rows], far_part[own_rows:]
    over_link = exchange(mine + exchange(other, 1), 2)
    near_part = near_pair()
    near_other = exchange(near_part[own_rows:].astype(jnp.bfloat16), 1)
    return near_part[:own_rows] + near_other + over_link


def swap_y(values):
    return lax.ppermute(values, "dp", [(i, i ^ 1) for i in range(8)])


def sum_line(kept):
    own_z = lax.axis_index("dp") // 2
    total = lax.dynamic_index_in_dim(kept, own_z, 0, keepdims=False).astype(jnp.float32)
    carried = {}
    for step in range(1, 4):
        for sign in (1, -1):
            target = jnp.clip(own_z + sign * (4 - step), 0, 3)
            block = lax.dynamic_index_in_dim(kept, target, 0, keepdims=False)
            if step > 1:
                block = block + carried[sign]
            senders = range(step) if sign > 0 else range(3, 3 - step, -1)
            pairs = [(2 * z + y, 2 * (z + sign) + y) for z in senders for y in range(2)]
            carried[sign] = lax.ppermute(block, "dp", pairs)
    return total + carried[1] + carried[-1]


def sum_clips(part, line_first=False):
    size = lax.axis_size("dp")
    part = part.astype(jnp.bfloat16)
    if size != 8:
        return lax.psum_scatter(part, "dp", scatter_dimension=0, tiled=True).astype(jnp.float32)
    own_y = lax.axis_index("dp") % 2
    halves = part.reshape(4, 2, part.shape[0] // 8, part.shape[1])
    if line_first:
        halves = sum_line(halves)[None]
    sent = lax.dynamic_index_in_dim(halves, 1 - own_y, 1, keepdims=False).astype(jnp.bfloat16)
    kept = lax.dynamic_index_in_dim(halves, own_y, 1, keepdims=False)
    kept = kept + swap_y(sent)
    return kept[0] if line_first else sum_line(kept)


def sum_everywhere(values):
    if lax.axis_size("dp") != 8:
        return lax.psum(values, ("dp", "tensor"))
    for flip in (1, 2):
        values = values + exchange(values, flip)
    for flip in (1, 2, 4):
        values = values + lax.ppermute(values, "dp", [(i, i ^ flip) for i in range(8)])
    return values


def after(values, *others):
    return lax.optimization_barrier((values,) + others)[0] if others else values


def attention_piece(q_block, k_ref, block_id, rows, cols, own_id, masked):
    keys = k_ref[pl.ds(pl.multiple_of((block_id ^ own_id) * rows, rows), rows), cols]
    scores = contract_cols(q_block, keys)
    if masked:
        row_ids = lax.broadcasted_iota(jnp.int32, (rows, rows), 0)
        col_ids = lax.broadcasted_iota(jnp.int32, (rows, rows), 1)
        scores = jnp.where(col_ids <= row_ids, scores, -1e30)
    return scores


def attention_weights(q_block, k_ref, block_id, rows, cols, own_id):
    pieces = [
        attention_piece(q_block, k_ref, other, rows, cols, own_id, other == block_id)
        for other in range(block_id + 1)
    ]
    peak = pieces[0].max(axis=1, keepdims=True)
    for piece in pieces[1:]:
        peak = jnp.maximum(peak, piece.max(axis=1, keepdims=True))
    pieces = [jnp.exp(piece - peak) for piece in pieces]
    total = pieces[0].sum(axis=1, keepdims=True)
    for piece in pieces[1:]:
        total = total + piece.sum(axis=1, keepdims=True)
    share = 1.0 / total
    return [piece * share for piece in pieces]


def forward_kernel(rows, id_ref, q_ref, k_ref, v_ref, out_ref):
    own_id = id_ref[0]
    for head in range(q_ref.shape[1] // HD):
        cols = slice(head * HD, (head + 1) * HD)
        for block_id in range(4):
            here = pl.ds(pl.multiple_of((block_id ^ own_id) * rows, rows), rows)
            q_block = q_ref[here, cols] * jnp.bfloat16(HD**-0.5)
            weights = attention_weights(q_block, k_ref, block_id, rows, cols, own_id)
            mixed = jnp.zeros((rows, HD), jnp.float32)
            for other, piece in enumerate(weights):
                there = pl.ds(pl.multiple_of((other ^ own_id) * rows, rows), rows)
                mixed = mixed + product(piece.astype(jnp.bfloat16), v_ref[there, cols])
            out_ref[here, cols] = mixed.astype(jnp.bfloat16)


def backward_kernel(
    rows, id_ref, q_ref, k_ref, v_ref, grad_ref, dq_ref, dk_ref, dv_ref, dk_sum, dv_sum
):
    own_id = id_ref[0]
    for head in range(q_ref.shape[1] // HD):
        cols = slice(head * HD, (head + 1) * HD)
        for block_id in range(3, -1, -1):
            here = pl.ds(pl.multiple_of((block_id ^ own_id) * rows, rows), rows)
            q_block = q_ref[here, cols] * jnp.bfloat16(HD**-0.5)
            grads = grad_ref[here, cols]
            weights = attention_weights(q_block, k_ref, block_id, rows, cols, own_id)
            theres = [
                pl.ds(pl.multiple_of((other ^ own_id) * rows, rows), rows)
                for other in range(block_id + 1)
            ]
            weight_grads = [contract_cols(grads, v_ref[there, cols]) for there in theres]
            row_dot = jnp.zeros((rows, 1), jnp.float32)
            for piece, piece_grad in zip(weights, weight_grads):
                row_dot = row_dot + (piece * piece_grad).sum(axis=1, keepdims=True)
            dq = jnp.zeros((rows, HD), jnp.float32)
            for other, there in enumerate(theres):
                piece = weights[other]
                score_grad = (piece * (weight_grads[other] - row_dot)).astype(jnp.bfloat16)
                dq = dq + product(score_grad, k_ref[there, cols])
                dk = contract_rows(score_grad, q_block)
                dv = contract_rows(piece.astype(jnp.bfloat16), grads)
                held = pl.ds(other * rows, rows)
                if block_id == 3:
                    dk_sum[held, cols] = dk
                    dv_sum[held, cols] = dv
                else:
                    dk_sum[held, cols] += dk
                    dv_sum[held, cols] += dv
            dq_ref[here, cols] = (dq * HD**-0.5).astype(jnp.bfloat16)
    for block_id in range(4):
        here = pl.ds(pl.multiple_of((block_id ^ own_id) * rows, rows), rows)
        dk_ref[here, :] = dk_sum[pl.ds(block_id * rows, rows), :].astype(jnp.bfloat16)
        dv_ref[here, :] = dv_sum[pl.ds(block_id * rows, rows), :].astype(jnp.bfloat16)


def pair_spec(length, first):
    return pl.BlockSpec((length, 2 * HD), lambda i, ids: (0, first + i))


def self_forward(qkv, own_id, rows):
    length, pairs = qkv.shape[0], qkv.shape[1] // (6 * HD)
    return pl.pallas_call(
        partial(forward_kernel, rows),
        out_shape=jax.ShapeDtypeStruct((length, pairs * 2 * HD), jnp.bfloat16),
        grid_spec=pltpu.PrefetchScalarGridSpec(
            num_scalar_prefetch=1,
            grid=(pairs,),
            in_specs=[pair_spec(length, part * pairs) for part in range(3)],
            out_specs=pair_spec(length, 0),
        ),
        cost_estimate=pl.CostEstimate(
            flops=pairs * 8 * HD * length * length * 5 // 8,
            bytes_accessed=pairs * 16 * HD * length,
            transcendentals=pairs * 2 * length * length * 5 // 8,
        ),
        name="self_forward",
    )(own_id.reshape(1), qkv, qkv, qkv)


def self_backward(qkv, grads, own_id, rows):
    length, pairs = qkv.shape[0], qkv.shape[1] // (6 * HD)
    return pl.pallas_call(
        partial(backward_kernel, rows),
        out_shape=[jax.ShapeDtypeStruct((length, pairs * 2 * HD), jnp.bfloat16)] * 3,
        grid_spec=pltpu.PrefetchScalarGridSpec(
            num_scalar_prefetch=1,
            grid=(pairs,),
            in_specs=[pair_spec(length, part * pairs) for part in range(3)]
            + [pair_spec(length, 0)],
            out_specs=[pair_spec(length, 0)] * 3,
            scratch_shapes=[pltpu.VMEM((length, 2 * HD), jnp.float32)] * 2,
        ),
        cost_estimate=pl.CostEstimate(
            flops=pairs * 20 * HD * length * length * 5 // 8,
            bytes_accessed=pairs * 28 * HD * length,
            transcendentals=pairs * 2 * length * length * 5 // 8,
        ),
        name="self_backward",
    )(own_id.reshape(1), qkv, qkv, qkv, grads)


def cross_forward(queries, all_keys, all_values):
    scores = jnp.einsum(
        "cqhd,ckhd->chqk", queries, all_keys, preferred_element_type=jnp.float32
    ) * HD ** (-0.5)
    row_peak = jnp.max(scores, axis=-1, keepdims=True)
    exp_scores = jnp.exp(scores - row_peak)
    weights = exp_scores / jnp.sum(exp_scores, axis=-1, keepdims=True)
    mixed_out = jnp.einsum(
        "chqk,ckhd->cqhd",
        weights.astype(jnp.bfloat16),
        all_values,
        preferred_element_type=jnp.float32,
    )
    return (mixed_out, weights)


def cross_backward(queries, all_keys, all_values, weights, grad_mixed):
    score_scale = HD ** (-0.5)
    grad_weights = jnp.einsum(
        "cqhd,ckhd->chqk", grad_mixed, all_values, preferred_element_type=jnp.float32
    )
    row_dot = jnp.sum(weights * grad_weights, axis=-1, keepdims=True)
    grad_scores = (weights * (grad_weights - row_dot)).astype(jnp.bfloat16)
    grad_queries = (
        jnp.einsum("chqk,ckhd->cqhd", grad_scores, all_keys, preferred_element_type=jnp.float32)
        * score_scale
    )
    grad_keys = (
        jnp.einsum("chqk,cqhd->ckhd", grad_scores, queries, preferred_element_type=jnp.float32)
        * score_scale
    )
    grad_values = jnp.einsum(
        "chqk,cqhd->ckhd",
        weights.astype(jnp.bfloat16),
        grad_mixed,
        preferred_element_type=jnp.float32,
    )
    return (grad_queries, grad_keys, grad_values)


def layer(
    layer_input,
    text_states,
    ln1_gain,
    ln1_bias,
    w_q,
    w_k,
    w_v,
    w_o,
    ln2_gain,
    ln2_bias,
    c_q,
    c_k,
    c_v,
    c_o,
    ln3_gain,
    ln3_bias,
    w_in,
    w_out,
    out_cotangent,
):
    clip_count = text_states.shape[0]
    text_len = text_states.shape[1]
    own_rows, model_width = layer_input.shape
    local_width = w_q.shape[1]
    own_id = lax.axis_index("tensor")
    low = jnp.bfloat16

    def split_heads(matrix, length):
        return matrix.astype(low).reshape(1, length, matrix.shape[1] // HD, HD)

    def merge_heads(tensor_four):
        return tensor_four.reshape(tensor_four.shape[1], -1).astype(low)

    stream = layer_input.astype(jnp.float32)
    normed_one = layer_norm(stream, ln1_gain, ln1_bias).astype(low)
    one = gather_relative(normed_one)
    w_qkv = jnp.concatenate([w_q, w_k, w_v], axis=1)
    rows_one = jnp.concatenate(one)
    qkv = product(rows_one, w_qkv).astype(low)
    attended = self_forward(qkv, own_id, own_rows)
    branch_one = scatter_product(
        lambda: product(attended[2 * own_rows :], w_o),
        lambda: product(attended[: 2 * own_rows], w_o),
        own_rows,
    )

    c_q_full = jnp.concatenate(gather_relative(after(c_q, one[2])), axis=1)
    c_o_full = jnp.concatenate(gather_relative(after(c_o, one[2])), axis=0)
    text_rows = text_states.reshape(clip_count * text_len, model_width)
    text_kv = after(
        jnp.concatenate([product(text_rows, c_k), product(text_rows, c_v)]).astype(low), one[2]
    )
    text_kv = jnp.concatenate(gather_relative(text_kv), axis=1)
    text_keys = split_heads(text_kv[:text_len], text_len)
    text_values = split_heads(text_kv[text_len:], text_len)
    grad_rows = gather_relative(after(out_cotangent, c_o_full))
    grad_near = jnp.concatenate(grad_rows[:2])
    grad_far = jnp.concatenate(grad_rows[2:])

    hidden_one = stream + branch_one
    normed_two = layer_norm(hidden_one, ln2_gain, ln2_bias).astype(low)
    cross_queries = split_heads(product(normed_two, c_q_full), own_rows)
    mixed_two, cross_weights = cross_forward(cross_queries, text_keys, text_values)
    crossed = merge_heads(mixed_two)
    branch_two = product(crossed, c_o_full)
    hidden_two = hidden_one + branch_two
    normed_three = layer_norm(hidden_two, ln3_gain, ln3_bias).astype(low)

    three = gather_relative(normed_three)
    near_three = jnp.concatenate(three[:2])
    far_three = jnp.concatenate(three[2:])
    act_parts, pre_grads = [], []
    for rows, grads in ((near_three, grad_near), (far_three, grad_far)):
        pre_act = product(rows, w_in)
        gelu_value, gelu_back = jax.vjp(partial(jax.nn.gelu, approximate=False), pre_act)
        act_parts.append(gelu_value.astype(low))
        pre_grads.append(gelu_back(contract_cols(grads, w_out))[0].astype(low))
    grad_normed_three = scatter_product(
        lambda: contract_cols(pre_grads[1], w_in),
        lambda: contract_cols(pre_grads[0], w_in),
        own_rows,
    )
    w_out_part = contract_rows(grad_near, act_parts[0]) + contract_rows(grad_far, act_parts[1])
    w_in_part = contract_rows(near_three, pre_grads[0]) + contract_rows(far_three, pre_grads[1])

    grad_out = out_cotangent.astype(jnp.float32)
    norm_value, norm_back = jax.vjp(layer_norm, hidden_two, ln3_gain, ln3_bias)
    back_rows, ln3_gain_part, ln3_bias_part = norm_back(grad_normed_three)
    grad_two = grad_out + back_rows
    grad_two_low = grad_two.astype(low)
    grad_mixed_two = split_heads(contract_cols(grad_two_low, c_o_full), own_rows)
    grad_cq, grad_tk, grad_tv = cross_backward(
        cross_queries, text_keys, text_values, cross_weights, grad_mixed_two
    )
    grad_cq = merge_heads(grad_cq)
    grad_normed_two = contract_cols(grad_cq, c_q_full)
    norm_value, norm_back = jax.vjp(layer_norm, hidden_one, ln2_gain, ln2_bias)
    back_rows, ln2_gain_part, ln2_bias_part = norm_back(grad_normed_two)
    grad_one = grad_two + back_rows

    one_grads = gather_relative(grad_one.astype(low))
    grad_one_rows = jnp.concatenate(one_grads)
    arrived = one_grads[3]
    branch_three = scatter_product(
        lambda: product(after(act_parts[1], arrived), w_out),
        lambda: product(act_parts[0], w_out),
        own_rows,
    )
    grad_mixed_one = contract_cols(grad_one_rows, w_o).astype(low)
    qkv_grads = self_backward(qkv, grad_mixed_one, own_id, own_rows)
    grad_qkv = jnp.concatenate(qkv_grads, axis=1)
    grad_normed_one = scatter_product(
        lambda: contract_cols(grad_qkv[2 * own_rows :], w_qkv),
        lambda: contract_cols(grad_qkv[: 2 * own_rows], w_qkv),
        own_rows,
    )
    w_out_grad = sum_clips(w_out_part).T
    w_in_grad = sum_clips(w_in_part, line_first=True)
    w_qkv_part = contract_rows(rows_one, grad_qkv)
    qkv_grad = sum_clips(w_qkv_part)
    w_q_grad, w_k_grad, w_v_grad = jnp.split(qkv_grad, 3, axis=1)
    norm_value, norm_back = jax.vjp(layer_norm, stream, ln1_gain, ln1_bias)
    back_rows, ln1_gain_part, ln1_bias_part = norm_back(grad_normed_one)
    input_grad = (grad_one + back_rows).astype(low)

    def columns(matrix):
        return [matrix[:, i * local_width : (i + 1) * local_width] for i in range(4)]

    rows_two = jnp.concatenate(gather_relative(after(normed_two, three[2])))
    crossed_rows = jnp.concatenate(swap_relative(columns(after(crossed, three[2]))))
    grad_two_rows = jnp.concatenate(gather_relative(grad_two_low))
    grad_cq_rows = jnp.concatenate(swap_relative(columns(after(grad_cq, one_grads[2]))))
    grad_text = jnp.concatenate(
        [part.reshape(text_len, -1) for part in (grad_tk, grad_tv)]
    ).astype(jnp.float32)
    grad_text = scatter_relative(*columns(grad_text)).astype(low)
    grad_tk, grad_tv = grad_text[:text_len], grad_text[text_len:]
    back_grad = sum_clips(
        jnp.concatenate(
            [
                contract_rows(grad_two_rows, crossed_rows).astype(low),
                contract_rows(grad_one_rows, attended).astype(low),
            ],
            axis=1,
        ),
    )
    cross_grad = sum_clips(
        jnp.concatenate(
            [
                contract_rows(rows_two, grad_cq_rows).astype(low),
                contract_rows(text_rows, grad_tk).astype(low),
                contract_rows(text_rows, grad_tv).astype(low),
            ],
            axis=1,
        ),
    )
    c_o_grad, w_o_grad = [part.T for part in jnp.split(back_grad, 2, axis=1)]
    c_q_grad, c_k_grad, c_v_grad = jnp.split(cross_grad, 3, axis=1)
    text_term = (contract_cols(grad_tk, c_k) + contract_cols(grad_tv, c_v)).astype(low)
    text_states_grad = (
        scatter_relative(
            *[
                lax.dynamic_slice_in_dim(text_term, (own_id ^ flip) * local_width, local_width, 1)
                for flip in range(4)
            ]
        )
        .astype(low)
        .reshape(clip_count, text_len, local_width)
    )

    block_out = (hidden_two + branch_three).astype(low)
    squares = jnp.stack(
        [
            jnp.sum(stream * stream),
            jnp.sum(branch_one * branch_one),
            jnp.sum(branch_two * branch_two),
            jnp.sum(branch_three * branch_three),
        ]
    )

    early = sum_everywhere(
        jnp.concatenate(
            [ln3_gain_part, ln3_bias_part, ln2_gain_part, ln2_bias_part, jnp.pad(squares, (0, 124))]
        )
    )
    late = sum_everywhere(jnp.concatenate([ln1_gain_part, ln1_bias_part]))
    ln3_gain_grad, ln3_bias_grad, ln2_gain_grad, ln2_bias_grad = [
        early[i * model_width : (i + 1) * model_width] for i in range(4)
    ]
    ln1_gain_grad, ln1_bias_grad = late[:model_width], late[model_width:]
    square_totals = early[4 * model_width : 4 * model_width + 4]
    entry_count = own_rows * lax.axis_size("dp") * lax.axis_size("tensor") * model_width
    root_squares = jnp.sqrt(square_totals / entry_count)
    return (
        block_out,
        input_grad,
        text_states_grad,
        ln1_gain_grad,
        ln1_bias_grad,
        w_q_grad,
        w_k_grad,
        w_v_grad,
        w_o_grad,
        ln2_gain_grad,
        ln2_bias_grad,
        c_q_grad,
        c_k_grad,
        c_v_grad,
        c_o_grad,
        ln3_gain_grad,
        ln3_bias_grad,
        w_in_grad,
        w_out_grad,
        root_squares,
    )


def solution(mesh):
    return jax.shard_map(
        layer,
        mesh=mesh,
        in_specs=(
            P(("dp", "tensor"), None),
            P("dp", None, None),
            P(),
            P(),
            P(None, "tensor"),
            P(None, "tensor"),
            P(None, "tensor"),
            P("tensor", None),
            P(),
            P(),
            P(None, "tensor"),
            P(None, "tensor"),
            P(None, "tensor"),
            P("tensor", None),
            P(),
            P(),
            P(None, "tensor"),
            P("tensor", None),
            P(("dp", "tensor"), None),
        ),
        out_specs=(
            P(("dp", "tensor"), None),
            P(("dp", "tensor"), None),
            P("dp", None, "tensor"),
            P(),
            P(),
            P("dp", "tensor"),
            P("dp", "tensor"),
            P("dp", "tensor"),
            P("tensor", "dp"),
            P(),
            P(),
            P("dp", "tensor"),
            P("dp", "tensor"),
            P("dp", "tensor"),
            P("tensor", "dp"),
            P(),
            P(),
            P("dp", "tensor"),
            P("tensor", "dp"),
            P(),
        ),
        check_vma=False,
    )
```

```python
from functools import partial

import jax
import jax.numpy as jnp
from jax import lax
from jax.experimental import pallas as pl
from jax.experimental.pallas import tpu as pltpu
from jax.sharding import PartitionSpec as P


HD = 64


norm_eps = 1e-05


def layer_norm(stream, gain_vec, shift_vec):
    centre = jnp.mean(stream, axis=-1, keepdims=True)
    centred = stream - centre
    spread = jnp.mean(centred * centred, axis=-1, keepdims=True)
    return centred * lax.rsqrt(spread + norm_eps) * gain_vec + shift_vec


def product(left_mat, right_mat):
    return jnp.dot(left_mat, right_mat, preferred_element_type=jnp.float32)


def contract_rows(left_mat, right_mat):
    return lax.dot_general(
        left_mat, right_mat, (((0,), (0,)), ((), ())), preferred_element_type=jnp.float32
    )


def contract_cols(left_mat, right_mat):
    return lax.dot_general(
        left_mat, right_mat, (((1,), (1,)), ((), ())), preferred_element_type=jnp.float32
    )


def exchange(values, flip):
    return lax.ppermute(values, "tensor", [(i, i ^ flip) for i in range(4)])


def gather_relative(values):
    far = exchange(values, 2)
    return values, exchange(values, 1), far, exchange(far, 1)


def scatter_relative(near_own, near_other, far_mine, far_other):
    over_link = exchange(far_mine + exchange(far_other, 1), 2)
    return near_own.astype(jnp.float32) + exchange(near_other, 1) + over_link


def gather_weight(values, axis):
    if lax.axis_size("dp") != 8:
        return jnp.concatenate(gather_relative(values), axis=axis)
    own_y = lax.axis_index("dp") % 2
    half = values.shape[0] // 2
    first = exchange(lax.dynamic_slice_in_dim(values, own_y * half, half, 0), 2)
    second = swap_y(first)
    far = jnp.concatenate(
        [jnp.where(own_y == 0, first, second), jnp.where(own_y == 0, second, first)]
    )
    return jnp.concatenate([values, exchange(values, 1), far, exchange(far, 1)], axis=axis)


def swap_relative(blocks):
    return [blocks[0]] + [exchange(blocks[flip], flip) for flip in (1, 2, 3)]


def scatter_product(far_pair, near_pair, own_rows):
    far_part = far_pair().astype(jnp.bfloat16)
    mine, other = far_part[:own_rows], far_part[own_rows:]
    both_mine = mine + exchange(other, 1)
    over_link = exchange(both_mine, 2)
    near_part = near_pair()
    near_other = exchange(near_part[own_rows:].astype(jnp.bfloat16), 1)
    return near_part[:own_rows] + near_other + over_link


def swap_y(values):
    return lax.ppermute(values, "dp", [(i, i ^ 1) for i in range(8)])


def sum_line(kept, axis):
    own_z = lax.axis_index("dp") // 2
    total = lax.dynamic_index_in_dim(kept, own_z, axis, keepdims=False).astype(jnp.float32)
    carried = None
    for step in range(1, 4):
        blocks = []
        for sign in (1, -1):
            target = jnp.clip(own_z + sign * (4 - step), 0, 3)
            blocks.append(lax.dynamic_index_in_dim(kept, target, axis, keepdims=False))
        if carried is not None:
            carried = lax.optimization_barrier(carried)
            blocks = [block + held for block, held in zip(blocks, carried)]
        blocks = lax.optimization_barrier(tuple(blocks))
        carried = []
        for block, sign in zip(blocks, (1, -1)):
            senders = range(step) if sign > 0 else range(3, 3 - step, -1)
            pairs = [(2 * z + y, 2 * (z + sign) + y) for z in senders for y in range(2)]
            carried.append(lax.ppermute(block, "dp", pairs))
        carried = tuple(carried)
    return total + carried[0] + carried[1]


def sum_clips(parts, line_first=False):
    size = lax.axis_size("dp")
    parts = [part.astype(jnp.bfloat16) for part in parts]
    if size != 8:
        return jnp.stack(
            [
                lax.psum_scatter(part, "dp", scatter_dimension=0, tiled=True).astype(jnp.float32)
                for part in parts
            ]
        )
    own_y = lax.axis_index("dp") % 2
    rows, width = parts[0].shape[0] // 8, parts[0].shape[1]
    if line_first:
        halves = [sum_line(parts[0].reshape(4, 2, rows, width), 0)[None]]
    else:
        halves = [part.reshape(4, 2, rows, width) for part in parts]

    def pick(place, kind):
        return jnp.stack(
            [lax.dynamic_index_in_dim(half, place, 1, keepdims=False).astype(kind) for half in halves]
        )

    other = swap_y(pick(1 - own_y, jnp.bfloat16))
    kept = pick(own_y, halves[0].dtype) + other
    return kept[0] if line_first else sum_line(kept, 1)


def sum_everywhere(values):
    if lax.axis_size("dp") != 8:
        return lax.psum(values, ("dp", "tensor"))
    for flip in (1, 2):
        values = values + exchange(values, flip)
    for flip in (2, 4, 1):
        values = values + lax.ppermute(values, "dp", [(i, i ^ flip) for i in range(8)])
    return values


def after(values, *others):
    return lax.optimization_barrier((values,) + others)[0] if others else values


def attention_piece(q_block, k_ref, block_id, rows, cols, own_id, masked):
    keys = k_ref[pl.ds(pl.multiple_of((block_id ^ own_id) * rows, rows), rows), cols]
    scores = contract_cols(q_block, keys)
    if masked:
        row_ids = lax.broadcasted_iota(jnp.int32, (rows, rows), 0)
        col_ids = lax.broadcasted_iota(jnp.int32, (rows, rows), 1)
        scores = jnp.where(col_ids <= row_ids, scores, -1e30)
    return scores


def attention_weights(q_block, k_ref, block_id, rows, cols, own_id):
    pieces = [
        attention_piece(q_block, k_ref, other, rows, cols, own_id, other == block_id)
        for other in range(block_id + 1)
    ]
    peak = pieces[0].max(axis=1, keepdims=True)
    for piece in pieces[1:]:
        peak = jnp.maximum(peak, piece.max(axis=1, keepdims=True))
    pieces = [jnp.exp(piece - peak) for piece in pieces]
    total = pieces[0].sum(axis=1, keepdims=True)
    for piece in pieces[1:]:
        total = total + piece.sum(axis=1, keepdims=True)
    share = 1.0 / total
    return [piece * share for piece in pieces]


def forward_kernel(rows, id_ref, q_ref, k_ref, v_ref, out_ref):
    own_id = id_ref[0]
    for head in range(q_ref.shape[1] // HD):
        cols = slice(head * HD, (head + 1) * HD)
        for block_id in range(4):
            here = pl.ds(pl.multiple_of((block_id ^ own_id) * rows, rows), rows)
            q_block = q_ref[here, cols] * jnp.bfloat16(HD**-0.5)
            weights = attention_weights(q_block, k_ref, block_id, rows, cols, own_id)
            mixed = jnp.zeros((rows, HD), jnp.float32)
            for other, piece in enumerate(weights):
                there = pl.ds(pl.multiple_of((other ^ own_id) * rows, rows), rows)
                mixed = mixed + product(piece.astype(jnp.bfloat16), v_ref[there, cols])
            out_ref[here, cols] = mixed.astype(jnp.bfloat16)


def backward_kernel(
    rows, id_ref, q_ref, k_ref, v_ref, grad_ref, dq_ref, dk_ref, dv_ref, dk_sum, dv_sum
):
    own_id = id_ref[0]
    for head in range(q_ref.shape[1] // HD):
        cols = slice(head * HD, (head + 1) * HD)
        for block_id in range(3, -1, -1):
            here = pl.ds(pl.multiple_of((block_id ^ own_id) * rows, rows), rows)
            q_block = q_ref[here, cols] * jnp.bfloat16(HD**-0.5)
            grads = grad_ref[here, cols]
            weights = attention_weights(q_block, k_ref, block_id, rows, cols, own_id)
            theres = [
                pl.ds(pl.multiple_of((other ^ own_id) * rows, rows), rows)
                for other in range(block_id + 1)
            ]
            weight_grads = [contract_cols(grads, v_ref[there, cols]) for there in theres]
            row_dot = jnp.zeros((rows, 1), jnp.float32)
            for piece, piece_grad in zip(weights, weight_grads):
                row_dot = row_dot + (piece * piece_grad).sum(axis=1, keepdims=True)
            dq = jnp.zeros((rows, HD), jnp.float32)
            for other, there in enumerate(theres):
                piece = weights[other]
                score_grad = (piece * (weight_grads[other] - row_dot)).astype(jnp.bfloat16)
                dq = dq + product(score_grad, k_ref[there, cols])
                dk = contract_rows(score_grad, q_block)
                dv = contract_rows(piece.astype(jnp.bfloat16), grads)
                held = pl.ds(other * rows, rows)
                if block_id == 3:
                    dk_sum[held, cols] = dk
                    dv_sum[held, cols] = dv
                else:
                    dk_sum[held, cols] += dk
                    dv_sum[held, cols] += dv
            dq_ref[here, cols] = (dq * HD**-0.5).astype(jnp.bfloat16)
    for block_id in range(4):
        here = pl.ds(pl.multiple_of((block_id ^ own_id) * rows, rows), rows)
        dk_ref[here, :] = dk_sum[pl.ds(block_id * rows, rows), :].astype(jnp.bfloat16)
        dv_ref[here, :] = dv_sum[pl.ds(block_id * rows, rows), :].astype(jnp.bfloat16)


def pair_spec(length, first):
    return pl.BlockSpec((length, 2 * HD), lambda i, ids: (0, first + i))


def self_forward(qkv, own_id, rows):
    length, pairs = qkv.shape[0], qkv.shape[1] // (6 * HD)
    return pl.pallas_call(
        partial(forward_kernel, rows),
        out_shape=jax.ShapeDtypeStruct((length, pairs * 2 * HD), jnp.bfloat16),
        grid_spec=pltpu.PrefetchScalarGridSpec(
            num_scalar_prefetch=1,
            grid=(pairs,),
            in_specs=[pair_spec(length, part * pairs) for part in range(3)],
            out_specs=pair_spec(length, 0),
        ),
        cost_estimate=pl.CostEstimate(
            flops=pairs * 8 * HD * length * length * 5 // 8,
            bytes_accessed=pairs * 16 * HD * length,
            transcendentals=pairs * 2 * length * length * 5 // 8,
        ),
        name="self_forward",
    )(own_id.reshape(1), qkv, qkv, qkv)


def self_backward(qkv, grads, own_id, rows):
    length, pairs = qkv.shape[0], qkv.shape[1] // (6 * HD)
    return pl.pallas_call(
        partial(backward_kernel, rows),
        out_shape=[jax.ShapeDtypeStruct((length, pairs * 2 * HD), jnp.bfloat16)] * 3,
        grid_spec=pltpu.PrefetchScalarGridSpec(
            num_scalar_prefetch=1,
            grid=(pairs,),
            in_specs=[pair_spec(length, part * pairs) for part in range(3)]
            + [pair_spec(length, 0)],
            out_specs=[pair_spec(length, 0)] * 3,
            scratch_shapes=[pltpu.VMEM((length, 2 * HD), jnp.float32)] * 2,
        ),
        cost_estimate=pl.CostEstimate(
            flops=pairs * 20 * HD * length * length * 5 // 8,
            bytes_accessed=pairs * 28 * HD * length,
            transcendentals=pairs * 2 * length * length * 5 // 8,
        ),
        name="self_backward",
    )(own_id.reshape(1), qkv, qkv, qkv, grads)


def cross_forward(queries, all_keys, all_values):
    scores = jnp.einsum(
        "cqhd,ckhd->chqk", queries, all_keys, preferred_element_type=jnp.float32
    ) * HD ** (-0.5)
    row_peak = jnp.max(scores, axis=-1, keepdims=True)
    exp_scores = jnp.exp(scores - row_peak)
    weights = exp_scores / jnp.sum(exp_scores, axis=-1, keepdims=True)
    mixed_out = jnp.einsum(
        "chqk,ckhd->cqhd",
        weights.astype(jnp.bfloat16),
        all_values,
        preferred_element_type=jnp.float32,
    )
    return (mixed_out, weights)


def cross_backward(queries, all_keys, all_values, weights, grad_mixed):
    score_scale = HD ** (-0.5)
    grad_weights = jnp.einsum(
        "cqhd,ckhd->chqk", grad_mixed, all_values, preferred_element_type=jnp.float32
    )
    row_dot = jnp.sum(weights * grad_weights, axis=-1, keepdims=True)
    grad_scores = (weights * (grad_weights - row_dot)).astype(jnp.bfloat16)
    grad_queries = (
        jnp.einsum("chqk,ckhd->cqhd", grad_scores, all_keys, preferred_element_type=jnp.float32)
        * score_scale
    )
    grad_keys = (
        jnp.einsum("chqk,cqhd->ckhd", grad_scores, queries, preferred_element_type=jnp.float32)
        * score_scale
    )
    grad_values = jnp.einsum(
        "chqk,cqhd->ckhd",
        weights.astype(jnp.bfloat16),
        grad_mixed,
        preferred_element_type=jnp.float32,
    )
    return (grad_queries, grad_keys, grad_values)


def layer(
    layer_input,
    text_states,
    ln1_gain,
    ln1_bias,
    w_q,
    w_k,
    w_v,
    w_o,
    ln2_gain,
    ln2_bias,
    c_q,
    c_k,
    c_v,
    c_o,
    ln3_gain,
    ln3_bias,
    w_in,
    w_out,
    out_cotangent,
):
    clip_count = text_states.shape[0]
    text_len = text_states.shape[1]
    own_rows, model_width = layer_input.shape
    local_width = w_q.shape[1]
    own_id = lax.axis_index("tensor")
    low = jnp.bfloat16

    def split_heads(matrix, length):
        return matrix.astype(low).reshape(1, length, matrix.shape[1] // HD, HD)

    def merge_heads(tensor_four):
        return tensor_four.reshape(tensor_four.shape[1], -1).astype(low)

    stream = layer_input.astype(jnp.float32)
    normed_one = layer_norm(stream, ln1_gain, ln1_bias).astype(low)
    one = gather_relative(normed_one)
    w_qkv = jnp.concatenate([w_q, w_k, w_v], axis=1)
    rows_one = jnp.concatenate(one)
    qkv = product(rows_one, w_qkv).astype(low)
    attended = self_forward(qkv, own_id, own_rows)
    branch_one = scatter_product(
        lambda: product(attended[2 * own_rows :], w_o),
        lambda: product(attended[: 2 * own_rows], w_o),
        own_rows,
    )

    c_q_full = gather_weight(after(c_q, one[2]), 1)
    c_o_full = gather_weight(after(c_o, one[2]), 0)
    text_rows = text_states.reshape(clip_count * text_len, model_width)
    text_kv = after(
        jnp.concatenate([product(text_rows, c_k), product(text_rows, c_v)]).astype(low), one[2]
    )
    text_kv = jnp.concatenate(gather_relative(text_kv), axis=1)
    text_keys = split_heads(text_kv[:text_len], text_len)
    text_values = split_heads(text_kv[text_len:], text_len)
    grad_rows = gather_relative(after(out_cotangent, branch_one))
    grad_near = jnp.concatenate(grad_rows[:2])
    grad_far = jnp.concatenate(grad_rows[2:])

    hidden_one = stream + branch_one
    normed_two = layer_norm(hidden_one, ln2_gain, ln2_bias).astype(low)
    cross_queries = split_heads(product(normed_two, c_q_full), own_rows)
    mixed_two, cross_weights = cross_forward(cross_queries, text_keys, text_values)
    crossed = merge_heads(mixed_two)
    branch_two = product(crossed, c_o_full)
    hidden_two = hidden_one + branch_two
    normed_three = layer_norm(hidden_two, ln3_gain, ln3_bias).astype(low)

    three = gather_relative(normed_three)
    near_three = jnp.concatenate(three[:2])
    far_three = jnp.concatenate(three[2:])
    act_parts, pre_grads = [], []
    for rows, grads in ((near_three, grad_near), (far_three, grad_far)):
        pre_act = product(rows, w_in)
        gelu_value, gelu_back = jax.vjp(partial(jax.nn.gelu, approximate=False), pre_act)
        act_parts.append(gelu_value.astype(low))
        pre_grads.append(gelu_back(contract_cols(grads, w_out))[0].astype(low))
    grad_normed_three = scatter_product(
        lambda: contract_cols(pre_grads[1], w_in),
        lambda: contract_cols(pre_grads[0], w_in),
        own_rows,
    )
    w_out_part = contract_rows(grad_near, act_parts[0]) + contract_rows(grad_far, act_parts[1])
    w_in_part = contract_rows(near_three, pre_grads[0]) + contract_rows(far_three, pre_grads[1])

    grad_out = out_cotangent.astype(jnp.float32)
    norm_value, norm_back = jax.vjp(layer_norm, hidden_two, ln3_gain, ln3_bias)
    back_rows, ln3_gain_part, ln3_bias_part = norm_back(grad_normed_three)
    grad_two = grad_out + back_rows
    grad_two_low = grad_two.astype(low)
    grad_mixed_two = split_heads(contract_cols(grad_two_low, c_o_full), own_rows)
    grad_cq, grad_tk, grad_tv = cross_backward(
        cross_queries, text_keys, text_values, cross_weights, grad_mixed_two
    )
    grad_cq = merge_heads(grad_cq)
    grad_normed_two = contract_cols(grad_cq, c_q_full)
    norm_value, norm_back = jax.vjp(layer_norm, hidden_one, ln2_gain, ln2_bias)
    back_rows, ln2_gain_part, ln2_bias_part = norm_back(grad_normed_two)
    grad_one = grad_two + back_rows

    one_grads = gather_relative(grad_one.astype(low))
    grad_one_rows = jnp.concatenate(one_grads)
    arrived = one_grads[3]
    branch_three = scatter_product(
        lambda: product(after(act_parts[1], arrived), w_out),
        lambda: product(act_parts[0], w_out),
        own_rows,
    )
    grad_mixed_one = contract_cols(grad_one_rows, w_o).astype(low)
    qkv_grads = self_backward(qkv, grad_mixed_one, own_id, own_rows)
    grad_qkv = jnp.concatenate(qkv_grads, axis=1)
    grad_normed_one = scatter_product(
        lambda: contract_cols(grad_qkv[2 * own_rows :], w_qkv),
        lambda: contract_cols(grad_qkv[: 2 * own_rows], w_qkv),
        own_rows,
    )
    w_out_grad = sum_clips([w_out_part])[0].T
    w_in_grad = sum_clips([w_in_part], line_first=True)[0]
    w_qkv_part = contract_rows(rows_one, grad_qkv)
    qkv_grad = sum_clips([w_qkv_part])[0]
    w_q_grad, w_k_grad, w_v_grad = jnp.split(qkv_grad, 3, axis=1)
    norm_value, norm_back = jax.vjp(layer_norm, stream, ln1_gain, ln1_bias)
    back_rows, ln1_gain_part, ln1_bias_part = norm_back(grad_normed_one)
    input_grad = (grad_one + back_rows).astype(low)

    def columns(matrix):
        return [matrix[:, i * local_width : (i + 1) * local_width] for i in range(4)]

    rows_two = jnp.concatenate(gather_relative(after(normed_two, three[2])))
    crossed_rows = jnp.concatenate(swap_relative(columns(after(crossed, three[2]))))
    grad_two_rows = jnp.concatenate(gather_relative(grad_two_low))
    grad_cq_rows = jnp.concatenate(swap_relative(columns(grad_cq)))
    grad_text = jnp.concatenate(
        [part.reshape(text_len, -1) for part in (grad_tk, grad_tv)]
    ).astype(jnp.float32)
    grad_text = scatter_relative(*columns(grad_text)).astype(low)
    grad_tk, grad_tv = grad_text[:text_len], grad_text[text_len:]
    c_o_grad, w_o_grad, c_q_grad, c_k_grad, c_v_grad = sum_clips(
        [
            contract_rows(grad_two_rows, crossed_rows),
            contract_rows(grad_one_rows, attended),
            contract_rows(rows_two, grad_cq_rows),
            contract_rows(text_rows, grad_tk),
            contract_rows(text_rows, grad_tv),
        ],
    )
    c_o_grad, w_o_grad = c_o_grad.T, w_o_grad.T
    text_term = (contract_cols(grad_tk, c_k) + contract_cols(grad_tv, c_v)).astype(low)
    text_states_grad = (
        scatter_relative(
            *[
                lax.dynamic_slice_in_dim(text_term, (own_id ^ flip) * local_width, local_width, 1)
                for flip in range(4)
            ]
        )
        .astype(low)
        .reshape(clip_count, text_len, local_width)
    )

    block_out = (hidden_two + branch_three).astype(low)
    squares = jnp.stack(
        [
            jnp.sum(stream * stream),
            jnp.sum(branch_one * branch_one),
            jnp.sum(branch_two * branch_two),
            jnp.sum(branch_three * branch_three),
        ]
    )

    totals = sum_everywhere(
        jnp.concatenate(
            [
                ln3_gain_part,
                ln3_bias_part,
                ln2_gain_part,
                ln2_bias_part,
                ln1_gain_part,
                ln1_bias_part,
                jnp.pad(squares, (0, 124)),
            ]
        ),
    )
    ln3_gain_grad, ln3_bias_grad, ln2_gain_grad, ln2_bias_grad, ln1_gain_grad, ln1_bias_grad = [
        totals[i * model_width : (i + 1) * model_width] for i in range(6)
    ]
    square_totals = totals[6 * model_width : 6 * model_width + 4]
    entry_count = own_rows * lax.axis_size("dp") * lax.axis_size("tensor") * model_width
    root_squares = jnp.sqrt(square_totals / entry_count)
    return (
        block_out,
        input_grad,
        text_states_grad,
        ln1_gain_grad,
        ln1_bias_grad,
        w_q_grad,
        w_k_grad,
        w_v_grad,
        w_o_grad,
        ln2_gain_grad,
        ln2_bias_grad,
        c_q_grad,
        c_k_grad,
        c_v_grad,
        c_o_grad,
        ln3_gain_grad,
        ln3_bias_grad,
        w_in_grad,
        w_out_grad,
        root_squares,
    )


def solution(mesh):
    return jax.shard_map(
        layer,
        mesh=mesh,
        in_specs=(
            P(("dp", "tensor"), None),
            P("dp", None, None),
            P(),
            P(),
            P(None, "tensor"),
            P(None, "tensor"),
            P(None, "tensor"),
            P("tensor", None),
            P(),
            P(),
            P(None, "tensor"),
            P(None, "tensor"),
            P(None, "tensor"),
            P("tensor", None),
            P(),
            P(),
            P(None, "tensor"),
            P("tensor", None),
            P(("dp", "tensor"), None),
        ),
        out_specs=(
            P(("dp", "tensor"), None),
            P(("dp", "tensor"), None),
            P("dp", None, "tensor"),
            P(),
            P(),
            P("dp", "tensor"),
            P("dp", "tensor"),
            P("dp", "tensor"),
            P("tensor", "dp"),
            P(),
            P(),
            P("dp", "tensor"),
            P("dp", "tensor"),
            P("dp", "tensor"),
            P("tensor", "dp"),
            P(),
            P(),
            P("dp", "tensor"),
            P("tensor", "dp"),
            P(),
        ),
        check_vma=False,
    )
```

```python
from functools import partial

import jax
import jax.numpy as jnp
from jax import lax
from jax.experimental import pallas as pl
from jax.experimental.pallas import tpu as pltpu
from jax.sharding import PartitionSpec as P


HD = 64


norm_eps = 1e-05


def layer_norm(stream, gain_vec, shift_vec):
    centre = jnp.mean(stream, axis=-1, keepdims=True)
    centred = stream - centre
    spread = jnp.mean(centred * centred, axis=-1, keepdims=True)
    return centred * lax.rsqrt(spread + norm_eps) * gain_vec + shift_vec


def product(left_mat, right_mat):
    return jnp.dot(left_mat, right_mat, preferred_element_type=jnp.float32)


def contract_rows(left_mat, right_mat):
    return lax.dot_general(
        left_mat, right_mat, (((0,), (0,)), ((), ())), preferred_element_type=jnp.float32
    )


def contract_cols(left_mat, right_mat):
    return lax.dot_general(
        left_mat, right_mat, (((1,), (1,)), ((), ())), preferred_element_type=jnp.float32
    )


def exchange(values, flip):
    return lax.ppermute(values, "tensor", [(i, i ^ flip) for i in range(4)])


def gather_relative(values):
    far = exchange(values, 2)
    return values, exchange(values, 1), far, exchange(far, 1)


def scatter_relative(near_own, near_other, far_mine, far_other):
    over_link = exchange(far_mine + exchange(far_other, 1), 2)
    return near_own.astype(jnp.float32) + exchange(near_other, 1) + over_link


def gather_weight(values, axis):
    if lax.axis_size("dp") != 8:
        return jnp.concatenate(gather_relative(values), axis=axis)
    own_y = lax.axis_index("dp") % 2
    half = values.shape[0] // 2
    first = exchange(lax.dynamic_slice_in_dim(values, own_y * half, half, 0), 2)
    second = swap_y(first)
    far = jnp.concatenate(
        [jnp.where(own_y == 0, first, second), jnp.where(own_y == 0, second, first)]
    )
    return jnp.concatenate([values, exchange(values, 1), far, exchange(far, 1)], axis=axis)


def swap_relative(blocks):
    return [blocks[0]] + [exchange(blocks[flip], flip) for flip in (1, 2, 3)]


def scatter_product(far_pair, near_pair, own_rows, held_by=None):
    far_part = far_pair().astype(jnp.bfloat16)
    mine, other = far_part[:own_rows], far_part[own_rows:]
    both_mine = mine + exchange(other, 1)
    over_link = exchange(both_mine, 2)
    near_part = near_pair()
    near_other = exchange(near_part[own_rows:].astype(jnp.bfloat16), 1)
    total = near_part[:own_rows] + near_other + over_link
    if held_by is None:
        return total
    return total + jnp.minimum(jnp.abs(held_by.astype(jnp.float32)), 0.0)


def swap_y(values):
    return lax.ppermute(values, "dp", [(i, i ^ 1) for i in range(8)])


def sum_line(kept, axis):
    own_z = lax.axis_index("dp") // 2
    total = lax.dynamic_index_in_dim(kept, own_z, axis, keepdims=False).astype(jnp.float32)
    carried = None
    for step in range(1, 4):
        blocks = []
        for sign in (1, -1):
            target = jnp.clip(own_z + sign * (4 - step), 0, 3)
            blocks.append(lax.dynamic_index_in_dim(kept, target, axis, keepdims=False))
        if carried is not None:
            carried = lax.optimization_barrier(carried)
            blocks = [block + held for block, held in zip(blocks, carried)]
        blocks = lax.optimization_barrier(tuple(blocks))
        carried = []
        for block, sign in zip(blocks, (1, -1)):
            senders = range(step) if sign > 0 else range(3, 3 - step, -1)
            pairs = [(2 * z + y, 2 * (z + sign) + y) for z in senders for y in range(2)]
            carried.append(lax.ppermute(block, "dp", pairs))
        carried = tuple(carried)
    return total + carried[0] + carried[1]


def sum_clips(parts, line_first=False):
    size = lax.axis_size("dp")
    parts = [part.astype(jnp.bfloat16) for part in parts]
    if size != 8:
        return jnp.stack(
            [
                lax.psum_scatter(part, "dp", scatter_dimension=0, tiled=True).astype(jnp.float32)
                for part in parts
            ]
        )
    own_y = lax.axis_index("dp") % 2
    rows, width = parts[0].shape[0] // 8, parts[0].shape[1]
    if line_first:
        halves = [sum_line(parts[0].reshape(4, 2, rows, width), 0)[None]]
    else:
        halves = [part.reshape(4, 2, rows, width) for part in parts]

    def pick(place, kind):
        return jnp.stack(
            [lax.dynamic_index_in_dim(half, place, 1, keepdims=False).astype(kind) for half in halves]
        )

    other = swap_y(pick(1 - own_y, jnp.bfloat16))
    kept = pick(own_y, halves[0].dtype) + other
    return kept[0] if line_first else sum_line(kept, 1)


def sum_everywhere(values):
    if lax.axis_size("dp") != 8:
        return lax.psum(values, ("dp", "tensor"))
    for flip in (1, 2):
        values = values + exchange(values, flip)
    for flip in (2, 4, 1):
        values = values + lax.ppermute(values, "dp", [(i, i ^ flip) for i in range(8)])
    return values


def after(values, *others):
    return lax.optimization_barrier((values,) + others)[0] if others else values


def attention_piece(q_block, k_ref, block_id, rows, cols, own_id, masked):
    keys = k_ref[pl.ds(pl.multiple_of((block_id ^ own_id) * rows, rows), rows), cols]
    scores = contract_cols(q_block, keys)
    if masked:
        row_ids = lax.broadcasted_iota(jnp.int32, (rows, rows), 0)
        col_ids = lax.broadcasted_iota(jnp.int32, (rows, rows), 1)
        scores = jnp.where(col_ids <= row_ids, scores, -1e30)
    return scores


def attention_weights(q_block, k_ref, block_id, rows, cols, own_id):
    pieces = [
        attention_piece(q_block, k_ref, other, rows, cols, own_id, other == block_id)
        for other in range(block_id + 1)
    ]
    peak = pieces[0].max(axis=1, keepdims=True)
    for piece in pieces[1:]:
        peak = jnp.maximum(peak, piece.max(axis=1, keepdims=True))
    pieces = [jnp.exp(piece - peak) for piece in pieces]
    total = pieces[0].sum(axis=1, keepdims=True)
    for piece in pieces[1:]:
        total = total + piece.sum(axis=1, keepdims=True)
    share = 1.0 / total
    return [piece * share for piece in pieces]


def forward_kernel(rows, id_ref, q_ref, k_ref, v_ref, out_ref):
    own_id = id_ref[0]
    for head in range(q_ref.shape[1] // HD):
        cols = slice(head * HD, (head + 1) * HD)
        for block_id in range(4):
            here = pl.ds(pl.multiple_of((block_id ^ own_id) * rows, rows), rows)
            q_block = q_ref[here, cols] * jnp.bfloat16(HD**-0.5)
            weights = attention_weights(q_block, k_ref, block_id, rows, cols, own_id)
            mixed = jnp.zeros((rows, HD), jnp.float32)
            for other, piece in enumerate(weights):
                there = pl.ds(pl.multiple_of((other ^ own_id) * rows, rows), rows)
                mixed = mixed + product(piece.astype(jnp.bfloat16), v_ref[there, cols])
            out_ref[here, cols] = mixed.astype(jnp.bfloat16)


def backward_kernel(
    rows, id_ref, q_ref, k_ref, v_ref, grad_ref, dq_ref, dk_ref, dv_ref, dk_sum, dv_sum
):
    own_id = id_ref[0]
    for head in range(q_ref.shape[1] // HD):
        cols = slice(head * HD, (head + 1) * HD)
        for block_id in range(3, -1, -1):
            here = pl.ds(pl.multiple_of((block_id ^ own_id) * rows, rows), rows)
            q_block = q_ref[here, cols] * jnp.bfloat16(HD**-0.5)
            grads = grad_ref[here, cols]
            weights = attention_weights(q_block, k_ref, block_id, rows, cols, own_id)
            theres = [
                pl.ds(pl.multiple_of((other ^ own_id) * rows, rows), rows)
                for other in range(block_id + 1)
            ]
            weight_grads = [contract_cols(grads, v_ref[there, cols]) for there in theres]
            row_dot = jnp.zeros((rows, 1), jnp.float32)
            for piece, piece_grad in zip(weights, weight_grads):
                row_dot = row_dot + (piece * piece_grad).sum(axis=1, keepdims=True)
            dq = jnp.zeros((rows, HD), jnp.float32)
            for other, there in enumerate(theres):
                piece = weights[other]
                score_grad = (piece * (weight_grads[other] - row_dot)).astype(jnp.bfloat16)
                dq = dq + product(score_grad, k_ref[there, cols])
                dk = contract_rows(score_grad, q_block)
                dv = contract_rows(piece.astype(jnp.bfloat16), grads)
                held = pl.ds(other * rows, rows)
                if block_id == 3:
                    dk_sum[held, cols] = dk
                    dv_sum[held, cols] = dv
                else:
                    dk_sum[held, cols] += dk
                    dv_sum[held, cols] += dv
            dq_ref[here, cols] = (dq * HD**-0.5).astype(jnp.bfloat16)
    for block_id in range(4):
        here = pl.ds(pl.multiple_of((block_id ^ own_id) * rows, rows), rows)
        dk_ref[here, :] = dk_sum[pl.ds(block_id * rows, rows), :].astype(jnp.bfloat16)
        dv_ref[here, :] = dv_sum[pl.ds(block_id * rows, rows), :].astype(jnp.bfloat16)


def pair_spec(length, first):
    return pl.BlockSpec((length, 2 * HD), lambda i, ids: (0, first + i))


def self_forward(qkv, own_id, rows):
    length, pairs = qkv.shape[0], qkv.shape[1] // (6 * HD)
    return pl.pallas_call(
        partial(forward_kernel, rows),
        out_shape=jax.ShapeDtypeStruct((length, pairs * 2 * HD), jnp.bfloat16),
        grid_spec=pltpu.PrefetchScalarGridSpec(
            num_scalar_prefetch=1,
            grid=(pairs,),
            in_specs=[pair_spec(length, part * pairs) for part in range(3)],
            out_specs=pair_spec(length, 0),
        ),
        cost_estimate=pl.CostEstimate(
            flops=pairs * 8 * HD * length * length * 5 // 8,
            bytes_accessed=pairs * 16 * HD * length,
            transcendentals=pairs * 2 * length * length * 5 // 8,
        ),
        name="self_forward",
    )(own_id.reshape(1), qkv, qkv, qkv)


def self_backward(qkv, grads, own_id, rows):
    length, pairs = qkv.shape[0], qkv.shape[1] // (6 * HD)
    return pl.pallas_call(
        partial(backward_kernel, rows),
        out_shape=[jax.ShapeDtypeStruct((length, pairs * 2 * HD), jnp.bfloat16)] * 3,
        grid_spec=pltpu.PrefetchScalarGridSpec(
            num_scalar_prefetch=1,
            grid=(pairs,),
            in_specs=[pair_spec(length, part * pairs) for part in range(3)]
            + [pair_spec(length, 0)],
            out_specs=[pair_spec(length, 0)] * 3,
            scratch_shapes=[pltpu.VMEM((length, 2 * HD), jnp.float32)] * 2,
        ),
        cost_estimate=pl.CostEstimate(
            flops=pairs * 20 * HD * length * length * 5 // 8,
            bytes_accessed=pairs * 28 * HD * length,
            transcendentals=pairs * 2 * length * length * 5 // 8,
        ),
        name="self_backward",
    )(own_id.reshape(1), qkv, qkv, qkv, grads)


def cross_forward(queries, all_keys, all_values):
    scores = jnp.einsum(
        "cqhd,ckhd->chqk", queries, all_keys, preferred_element_type=jnp.float32
    ) * HD ** (-0.5)
    row_peak = jnp.max(scores, axis=-1, keepdims=True)
    exp_scores = jnp.exp(scores - row_peak)
    weights = exp_scores / jnp.sum(exp_scores, axis=-1, keepdims=True)
    mixed_out = jnp.einsum(
        "chqk,ckhd->cqhd",
        weights.astype(jnp.bfloat16),
        all_values,
        preferred_element_type=jnp.float32,
    )
    return (mixed_out, weights)


def cross_backward(queries, all_keys, all_values, weights, grad_mixed):
    score_scale = HD ** (-0.5)
    grad_weights = jnp.einsum(
        "cqhd,ckhd->chqk", grad_mixed, all_values, preferred_element_type=jnp.float32
    )
    row_dot = jnp.sum(weights * grad_weights, axis=-1, keepdims=True)
    grad_scores = (weights * (grad_weights - row_dot)).astype(jnp.bfloat16)
    grad_queries = (
        jnp.einsum("chqk,ckhd->cqhd", grad_scores, all_keys, preferred_element_type=jnp.float32)
        * score_scale
    )
    grad_keys = (
        jnp.einsum("chqk,cqhd->ckhd", grad_scores, queries, preferred_element_type=jnp.float32)
        * score_scale
    )
    grad_values = jnp.einsum(
        "chqk,cqhd->ckhd",
        weights.astype(jnp.bfloat16),
        grad_mixed,
        preferred_element_type=jnp.float32,
    )
    return (grad_queries, grad_keys, grad_values)


def layer(
    layer_input,
    text_states,
    ln1_gain,
    ln1_bias,
    w_q,
    w_k,
    w_v,
    w_o,
    ln2_gain,
    ln2_bias,
    c_q,
    c_k,
    c_v,
    c_o,
    ln3_gain,
    ln3_bias,
    w_in,
    w_out,
    out_cotangent,
):
    clip_count = text_states.shape[0]
    text_len = text_states.shape[1]
    own_rows, model_width = layer_input.shape
    local_width = w_q.shape[1]
    own_id = lax.axis_index("tensor")
    low = jnp.bfloat16

    def split_heads(matrix, length):
        return matrix.astype(low).reshape(1, length, matrix.shape[1] // HD, HD)

    def merge_heads(tensor_four):
        return tensor_four.reshape(tensor_four.shape[1], -1).astype(low)

    stream = layer_input.astype(jnp.float32)
    normed_one = layer_norm(stream, ln1_gain, ln1_bias).astype(low)
    one = gather_relative(normed_one)
    w_qkv = jnp.concatenate([w_q, w_k, w_v], axis=1)
    rows_one = jnp.concatenate(one)
    qkv = product(rows_one, w_qkv).astype(low)
    attended = self_forward(qkv, own_id, own_rows)
    branch_one = scatter_product(
        lambda: product(attended[2 * own_rows :], w_o),
        lambda: product(attended[: 2 * own_rows], w_o),
        own_rows,
    )

    c_q_full = gather_weight(after(c_q, one[2]), 1)
    c_o_full = gather_weight(after(c_o, one[2]), 0)
    text_rows = text_states.reshape(clip_count * text_len, model_width)
    text_kv = after(
        jnp.concatenate([product(text_rows, c_k), product(text_rows, c_v)]).astype(low), one[2]
    )
    text_kv = jnp.concatenate(gather_relative(text_kv), axis=1)
    text_keys = split_heads(text_kv[:text_len], text_len)
    text_values = split_heads(text_kv[text_len:], text_len)
    grad_rows = gather_relative(after(out_cotangent, branch_one))
    grad_near = jnp.concatenate(grad_rows[:2])
    grad_far = jnp.concatenate(grad_rows[2:])

    hidden_one = stream + branch_one
    normed_two = layer_norm(hidden_one, ln2_gain, ln2_bias).astype(low)
    cross_queries = split_heads(product(normed_two, c_q_full), own_rows)
    mixed_two, cross_weights = cross_forward(cross_queries, text_keys, text_values)
    crossed = merge_heads(mixed_two)
    branch_two = product(crossed, c_o_full)
    hidden_two = hidden_one + branch_two
    normed_three = layer_norm(hidden_two, ln3_gain, ln3_bias).astype(low)

    three = gather_relative(normed_three)
    near_three = jnp.concatenate(three[:2])
    far_three = jnp.concatenate(three[2:])
    act_parts, pre_grads = [], []
    for rows, grads in ((near_three, grad_near), (far_three, grad_far)):
        pre_act = product(rows, w_in)
        gelu_value, gelu_back = jax.vjp(partial(jax.nn.gelu, approximate=False), pre_act)
        act_parts.append(gelu_value.astype(low))
        pre_grads.append(gelu_back(contract_cols(grads, w_out))[0].astype(low))
    grad_normed_three = scatter_product(
        lambda: contract_cols(pre_grads[1], w_in),
        lambda: contract_cols(pre_grads[0], w_in),
        own_rows,
    )
    w_out_part = contract_rows(grad_near, act_parts[0]) + contract_rows(grad_far, act_parts[1])
    w_in_part = contract_rows(near_three, pre_grads[0]) + contract_rows(far_three, pre_grads[1])

    grad_out = out_cotangent.astype(jnp.float32)
    norm_value, norm_back = jax.vjp(layer_norm, hidden_two, ln3_gain, ln3_bias)
    back_rows, ln3_gain_part, ln3_bias_part = norm_back(grad_normed_three)
    grad_two = grad_out + back_rows
    grad_two_low = grad_two.astype(low)
    grad_mixed_two = split_heads(contract_cols(grad_two_low, c_o_full), own_rows)
    grad_cq, grad_tk, grad_tv = cross_backward(
        cross_queries, text_keys, text_values, cross_weights, grad_mixed_two
    )
    grad_cq = merge_heads(grad_cq)
    grad_normed_two = contract_cols(grad_cq, c_q_full)
    norm_value, norm_back = jax.vjp(layer_norm, hidden_one, ln2_gain, ln2_bias)
    back_rows, ln2_gain_part, ln2_bias_part = norm_back(grad_normed_two)
    grad_one = grad_two + back_rows

    one_grads = gather_relative(grad_one.astype(low))
    grad_one_rows = jnp.concatenate(one_grads)
    grad_mixed_one = contract_cols(grad_one_rows, w_o).astype(low)
    qkv_grads = self_backward(qkv, grad_mixed_one, own_id, own_rows)
    branch_three = scatter_product(
        lambda: product(act_parts[1], w_out),
        lambda: product(act_parts[0], w_out),
        own_rows,
        qkv_grads[0][0, 0],
    )
    grad_qkv = jnp.concatenate(qkv_grads, axis=1)
    grad_normed_one = scatter_product(
        lambda: contract_cols(grad_qkv[2 * own_rows :], w_qkv),
        lambda: contract_cols(grad_qkv[: 2 * own_rows], w_qkv),
        own_rows,
    )
    w_out_grad = sum_clips([w_out_part])[0].T
    w_in_grad = sum_clips([w_in_part], line_first=True)[0]
    w_qkv_part = contract_rows(rows_one, grad_qkv)
    qkv_grad = sum_clips([w_qkv_part])[0]
    w_q_grad, w_k_grad, w_v_grad = jnp.split(qkv_grad, 3, axis=1)
    norm_value, norm_back = jax.vjp(layer_norm, stream, ln1_gain, ln1_bias)
    back_rows, ln1_gain_part, ln1_bias_part = norm_back(grad_normed_one)
    input_grad = (grad_one + back_rows).astype(low)

    def columns(matrix):
        return [matrix[:, i * local_width : (i + 1) * local_width] for i in range(4)]

    rows_two = jnp.concatenate(gather_relative(after(normed_two, three[2])))
    crossed_rows = jnp.concatenate(swap_relative(columns(after(crossed, three[2]))))
    grad_two_rows = jnp.concatenate(gather_relative(grad_two_low))
    grad_cq_rows = jnp.concatenate(swap_relative(columns(grad_cq)))
    grad_text = jnp.concatenate(
        [part.reshape(text_len, -1) for part in (grad_tk, grad_tv)]
    ).astype(jnp.float32)
    grad_text = scatter_relative(*columns(grad_text)).astype(low)
    grad_tk, grad_tv = grad_text[:text_len], grad_text[text_len:]
    c_o_grad = sum_clips([contract_rows(grad_two_rows, crossed_rows)])[0]
    w_o_grad, c_q_grad, c_k_grad, c_v_grad = sum_clips(
        [
            contract_rows(grad_one_rows, attended),
            contract_rows(rows_two, grad_cq_rows),
            contract_rows(text_rows, grad_tk),
            contract_rows(text_rows, grad_tv),
        ],
    )
    c_o_grad, w_o_grad = c_o_grad.T, w_o_grad.T
    text_term = (contract_cols(grad_tk, c_k) + contract_cols(grad_tv, c_v)).astype(low)
    text_states_grad = (
        scatter_relative(
            *[
                lax.dynamic_slice_in_dim(text_term, (own_id ^ flip) * local_width, local_width, 1)
                for flip in range(4)
            ]
        )
        .astype(low)
        .reshape(clip_count, text_len, local_width)
    )

    block_out = (hidden_two + branch_three).astype(low)
    squares = jnp.stack(
        [
            jnp.sum(stream * stream),
            jnp.sum(branch_one * branch_one),
            jnp.sum(branch_two * branch_two),
            jnp.sum(branch_three * branch_three),
        ]
    )

    totals = sum_everywhere(
        jnp.concatenate(
            [
                ln3_gain_part,
                ln3_bias_part,
                ln2_gain_part,
                ln2_bias_part,
                ln1_gain_part,
                ln1_bias_part,
                jnp.pad(squares, (0, 124)),
            ]
        ),
    )
    ln3_gain_grad, ln3_bias_grad, ln2_gain_grad, ln2_bias_grad, ln1_gain_grad, ln1_bias_grad = [
        totals[i * model_width : (i + 1) * model_width] for i in range(6)
    ]
    square_totals = totals[6 * model_width : 6 * model_width + 4]
    entry_count = own_rows * lax.axis_size("dp") * lax.axis_size("tensor") * model_width
    root_squares = jnp.sqrt(square_totals / entry_count)
    return (
        block_out,
        input_grad,
        text_states_grad,
        ln1_gain_grad,
        ln1_bias_grad,
        w_q_grad,
        w_k_grad,
        w_v_grad,
        w_o_grad,
        ln2_gain_grad,
        ln2_bias_grad,
        c_q_grad,
        c_k_grad,
        c_v_grad,
        c_o_grad,
        ln3_gain_grad,
        ln3_bias_grad,
        w_in_grad,
        w_out_grad,
        root_squares,
    )


def solution(mesh):
    return jax.shard_map(
        layer,
        mesh=mesh,
        in_specs=(
            P(("dp", "tensor"), None),
            P("dp", None, None),
            P(),
            P(),
            P(None, "tensor"),
            P(None, "tensor"),
            P(None, "tensor"),
            P("tensor", None),
            P(),
            P(),
            P(None, "tensor"),
            P(None, "tensor"),
            P(None, "tensor"),
            P("tensor", None),
            P(),
            P(),
            P(None, "tensor"),
            P("tensor", None),
            P(("dp", "tensor"), None),
        ),
        out_specs=(
            P(("dp", "tensor"), None),
            P(("dp", "tensor"), None),
            P("dp", None, "tensor"),
            P(),
            P(),
            P("dp", "tensor"),
            P("dp", "tensor"),
            P("dp", "tensor"),
            P("tensor", "dp"),
            P(),
            P(),
            P("dp", "tensor"),
            P("dp", "tensor"),
            P("dp", "tensor"),
            P("tensor", "dp"),
            P(),
            P(),
            P("dp", "tensor"),
            P("tensor", "dp"),
            P(),
        ),
        check_vma=False,
    )
```
